16 devices in a mesh: rep: 2 (over y, z), dp: 8 (over x, core).
Axes of the slice: x: 4, y: 2, z: 1, core: 2. Of those that a mesh axis runs over, the one named last changes fastest.
The devices are a block of a 4x4x8 slice.
Arguments:
- g_w_gate: bfloat16 [16, 2, 896, 2304], P(('rep', 'dp')), parts along dimension 0
- g_w_up: bfloat16 [16, 2, 896, 2304], P(('rep', 'dp')), parts along dimension 0
- g_w_down: bfloat16 [16, 2, 2304, 896], P(('rep', 'dp')), parts along dimension 0
- w_gate: bfloat16 [2, 896, 2304], replicated
- w_up: bfloat16 [2, 896, 2304], replicated
- w_down: bfloat16 [2, 2304, 896], replicated
- m_w_gate: float32 [2, 896, 2304], P(None, 'dp')
- m_w_up: float32 [2, 896, 2304], P(None, 'dp')
- m_w_down: float32 [2, 2304, 896], P(None, 'dp')
- v_w_gate: float32 [2, 896, 2304], P(None, 'dp')
- v_w_up: float32 [2, 896, 2304], P(None, 'dp')
- v_w_down: float32 [2, 2304, 896], P(None, 'dp')
Outputs:
- output 1: bfloat16 [4, 896, 2304], P('rep'), parts along dimension 0
- output 2: bfloat16 [4, 896, 2304], P('rep'), parts along dimension 0
- output 3: bfloat16 [4, 2304, 896], P('rep'), parts along dimension 0
- output 4: float32 [4, 896, 2304], P('rep', 'dp'), parts along dimension 0
- output 5: float32 [4, 896, 2304], P('rep', 'dp'), parts along dimension 0
- output 6: float32 [4, 2304, 896], P('rep', 'dp'), parts along dimension 0
- output 7: float32 [4, 896, 2304], P('rep', 'dp'), parts along dimension 0
- output 8: float32 [4, 896, 2304], P('rep', 'dp'), parts along dimension 0
- output 9: float32 [4, 2304, 896], P('rep', 'dp'), parts along dimension 0
There are 2 independent parts. The reference program is written for one: setup_inputs(seed, part) draws one part's arguments, and reference() takes and returns one part's arrays. A program takes and returns all parts, laid end to end along the dimension named above; an argument that names none is the same for every part.
All inputs are finite; a program needn't handle non-finite values.
Results may differ from the reference program's by a relative error of at most 0.022.
Values are sent between devices in bfloat16 or wider.
A program may use at most 768 MiB of HBM per device.

```python
import jax
import jax.numpy as jnp
from jax import lax

DEVICES = 8
D = 896
FF = 2304
LAYERS = 2
NAMES = ("w_gate", "w_up", "w_down")
SHAPES = {"w_gate": (LAYERS, D, FF), "w_up": (LAYERS, D, FF), "w_down": (LAYERS, FF, D)}


def setup_inputs(seed: int = 0, part: int = 0) -> dict:
    kz, *keys = jax.random.split(jax.random.key(seed), 1 + 5 * len(NAMES))
    loud = 2.0 ** jax.random.uniform(kz, (), jnp.float32, -1.0, 1.0)
    drawn = {}
    for name, key, both in zip(NAMES, keys[:3], keys[3:6], strict=True):
        own = jax.random.normal(jax.random.fold_in(key, part), (DEVICES, *SHAPES[name]), jnp.float32)
        shared = jax.random.normal(jax.random.fold_in(both, part), SHAPES[name], jnp.float32)
        drawn["g_" + name] = (loud * (0.7 * shared / DEVICES + 0.7 * own * DEVICES**-0.5)).astype(jnp.bfloat16)
    for name, key in zip(NAMES, keys[6:9], strict=True):
        drawn[name] = (jax.random.normal(key, SHAPES[name], jnp.float32) * SHAPES[name][1] ** -0.5).astype(jnp.bfloat16)
    for name, key in zip(NAMES, keys[9:12], strict=True):
        drawn["m_" + name] = loud * 0.5 * jax.random.normal(key, SHAPES[name], jnp.float32)
    for name, key in zip(NAMES, keys[12:15], strict=True):
        drawn["v_" + name] = loud * loud * jax.random.uniform(key, SHAPES[name], jnp.float32, 0.5, 1.5)
    return drawn


def adamw(w, m, v, g):
    m = 0.9 * m + 0.1 * g
    v = 0.95 * v + 0.05 * g * g
    step = m * lax.rsqrt(v + 1e-8) + 0.1 * w
    return (w - 0.02 * step).astype(jnp.bfloat16), m, v


def clipped(gradients, sum_of_squares, count):
    factor = jnp.minimum(1.0, 0.5 * lax.rsqrt(sum_of_squares / count + 1e-30))
    return [g * factor for g in gradients]


def reference(g_w_gate, g_w_up, g_w_down, w_gate, w_up, w_down, m_w_gate, m_w_up, m_w_down, v_w_gate, v_w_up, v_w_down):
    def total(terms):
        return lax.scan(lambda so_far, term: (so_far + term.astype(jnp.float32), None), jnp.zeros(terms.shape[1:], jnp.float32), terms)[0]

    gradients = [total(terms).astype(jnp.bfloat16).astype(jnp.float32) for terms in (g_w_gate, g_w_up, g_w_down)]
    gradients = clipped(gradients, sum(jnp.sum(g * g) for g in gradients), sum(g.size for g in gradients))
    new = [
        adamw(w.astype(jnp.float32), m, v, g)
        for w, m, v, g in zip((w_gate, w_up, w_down), (m_w_gate, m_w_up, m_w_down), (v_w_gate, v_w_up, v_w_down), gradients, strict=True)
    ]
    return tuple(one[which] for which in range(3) for one in new)
```

```python
import functools

import jax
import jax.numpy as jnp
from jax import lax
from jax.experimental import pallas as pl
from jax.experimental.pallas import tpu as pltpu
from jax.sharding import PartitionSpec as P

LAYERS = 2
KINDS = 3
MESH = pl.DeviceIdType.MESH


def strip(columns):
    return 16 if columns > 1024 else 48


def tile_sum(x):
    tiles = [x[r : r + 8, c : c + 128] for r in range(0, x.shape[0], 8) for c in range(0, x.shape[1], 128)]
    while len(tiles) > 1:
        tiles = [a + b for a, b in zip(tiles[::2], tiles[1::2])] + ([tiles[-1]] if len(tiles) % 2 else [])
    return tiles[0]


def kernel(size, count, *refs):
    chips = size // 2
    take = iter(refs)
    some = lambda n: [next(take) for _ in range(n)]
    g_in, w_in, m_in, v_in = some(KINDS), some(KINDS), some(KINDS), some(KINDS)
    W, M, V = some(KINDS), some(KINDS), some(KINDS)
    old, hop, last = some(KINDS), some(KINDS), some(KINDS)
    squares, own_sem, load_sem, peer_send, peer_recv, link_send, link_recv, sq_send, sq_recv = some(9)

    me = lax.axis_index("dp")
    chip, core = me // 2, lax.rem(me, 2)
    at = lambda offset: lax.rem(chip + offset, chips)
    sibling = chip * 2 + 1 - core
    ahead, behind = at(1) * 2 + core, at(chips - 1) * 2 + core
    across = chips // 2
    offsets = (across, 1, chips - 1, 0)
    rows = [m.shape[1] for m in m_in]

    def block(a, device, start=0, height=None):
        return pl.ds(pl.multiple_of(device * rows[a] + start, 16), rows[a] if height is None else height)

    def unit(o, l, a):
        return (offsets.index(o) * LAYERS + l) * KINDS + a

    def mine(o):
        return at(o) * 2 + core

    def theirs(o):
        return at(o) * 2 + 1 - core

    own = {}
    for o in offsets:
        for a in range(KINDS):
            for l in range(LAYERS):
                place = W[a].at[l, block(a, mine(o))]
                own[o, l, a] = pltpu.make_async_copy(g_in[a].at[0, l, block(a, mine(o))], place, own_sem.at[unit(o, l, a)])
                own[o, l, a].start()

    barrier = pltpu.get_barrier_semaphore()
    for step in range(1, size):
        pl.semaphore_signal(barrier, inc=1, device_id={"dp": lax.rem(me + step, size)}, device_id_type=MESH)
    pl.semaphore_wait(barrier, size - 1)

    given = {}
    for o in offsets:
        for a in range(KINDS):
            for l in range(LAYERS):
                given[o, l, a] = pltpu.make_async_remote_copy(
                    g_in[a].at[0, l, block(a, theirs(o))],
                    W[a].at[l, block(a, mine(o))],
                    peer_send.at[unit(o, l, a)],
                    peer_recv.at[unit(o, l, a)],
                    device_id={"dp": sibling},
                    device_id_type=MESH,
                )
                given[o, l, a].start()

    loads = []
    for l in range(LAYERS):
        for a in range(KINDS):
            for n, (source, target) in enumerate(
                ((w_in[a].at[l, block(a, me)], old[a].at[l]), (m_in[a].at[l], M[a].at[l]), (v_in[a].at[l], V[a].at[l]))
            ):
                loads.append(pltpu.make_async_copy(source, target, load_sem.at[(l * KINDS + a) * 3 + n]))
                loads[-1].start()

    def each_strip(a, body, init):
        height = strip(g_in[a].shape[-1])
        return lax.fori_loop(0, rows[a] // height, lambda i, carry: body(pl.multiple_of(i * height, 16), height, carry), init)

    def add(o, l, a, more=()):
        own[o, l, a].wait()
        given[o, l, a].wait_recv()

        def body(start, height, carry):
            here = W[a].at[l, block(a, mine(o), start, height)]
            total = here[...].astype(jnp.float32) + W[a][l, block(a, theirs(o), start, height)].astype(jnp.float32)
            for other in more:
                total = total + other[pl.ds(start, height)].astype(jnp.float32)
            total = total.astype(jnp.bfloat16)
            here[...] = total
            if o == 0:
                total = total.astype(jnp.float32)
                carry = carry + tile_sum(total * total)
            return carry

        return each_strip(a, body, jnp.zeros((8, 128), jnp.float32) if o == 0 else 0)

    def to_link(source, target, slot, device):
        copy = pltpu.make_async_remote_copy(
            source, target, link_send.at[slot], link_recv.at[slot], device_id={"dp": device}, device_id_type=MESH
        )
        copy.start()
        return copy

    side = lambda forward: 0 if forward else 1
    slot = lambda forward, stage, a: (side(forward) * 3 + stage) * KINDS + a
    sent = {}
    for a in range(KINDS):
        for forward, l in ((True, 0), (False, 1)):
            add(across, l, a)
            sent[forward, 0, a] = to_link(
                W[a].at[l, block(a, mine(across))], hop[a].at[l], slot(forward, 0, a), ahead if forward else behind
            )
    for a in range(KINDS):
        for forward, l in ((True, 1), (False, 0)):
            o = 1 if forward else chips - 1
            add(o, l, a)
            sent[forward, 1, a] = to_link(
                W[a].at[l, block(a, mine(o))], last[a].at[side(forward), l], slot(forward, 1, a), ahead if forward else behind
            )
    for a in range(KINDS):
        for forward, l in ((True, 0), (False, 1)):
            o = 1 if forward else chips - 1
            sent[forward, 0, a].wait_recv()
            add(o, l, a, (hop[a].at[l],))
            sent[forward, 2, a] = to_link(
                W[a].at[l, block(a, mine(o))], last[a].at[side(forward), l], slot(forward, 2, a), ahead if forward else behind
            )
    total = jnp.zeros((8, 128), jnp.float32)
    for a in range(KINDS):
        for l in range(LAYERS):
            sent[True, 2 - l, a].wait_recv()
            sent[False, 1 + l, a].wait_recv()
            total = total + add(0, l, a, (last[a].at[0, l], last[a].at[1, l]))
    for copy in (*given.values(), *sent.values()):
        copy.wait_send()

    squares[me] = total
    told = []
    for step in range(1, size):
        told.append(
            pltpu.make_async_remote_copy(
                squares.at[me],
                squares.at[me],
                sq_send.at[step - 1],
                sq_recv.at[step - 1],
                device_id={"dp": lax.rem(me + step, size)},
                device_id_type=MESH,
            )
        )
        told[-1].start()
    for copy in loads:
        copy.wait()
    for copy in told:
        copy.wait_recv()
    everything = jnp.sum(jnp.sum(squares[...], axis=0), keepdims=True)
    factor = jnp.minimum(1.0, 0.5 * lax.rsqrt(everything / count + 1e-30))

    def update(l, a):
        def body(start, height, carry):
            here = W[a].at[l, block(a, me, start, height)]
            part = pl.ds(start, height)
            g = here[...].astype(jnp.float32) * factor
            w = old[a][l, part].astype(jnp.float32)
            m = 0.9 * M[a][l, part] + 0.1 * g
            v = 0.95 * V[a][l, part] + 0.05 * g * g
            M[a][l, part] = m
            V[a][l, part] = v
            here[...] = (w - 0.02 * (m * lax.rsqrt(v + 1e-8) + 0.1 * w)).astype(jnp.bfloat16)
            return carry

        each_strip(a, body, 0)

    def share(o, l, a):
        place = W[a].at[l, block(a, mine(o))]
        copy = pltpu.make_async_remote_copy(
            place, place, peer_send.at[unit(o, l, a)], peer_recv.at[unit(o, l, a)], device_id={"dp": sibling}, device_id_type=MESH
        )
        copy.start()
        return copy

    def pass_on(forward, stage, o, l, a):
        place = W[a].at[l, block(a, mine(o))]
        sent[forward, stage, a] = to_link(place, place, slot(forward, stage, a), ahead if forward else behind)

    shared = []
    for a in range(KINDS):
        for forward, l in ((True, 0), (False, 1)):
            update(l, a)
            pass_on(forward, 0, 0, l, a)
            shared.append(share(0, l, a))
    for a in range(KINDS):
        for forward, l in ((True, 1), (False, 0)):
            pass_on(forward, 1, 0, l, a)
    for stage in range(3):
        for a in range(KINDS):
            for forward, l in ((True, 0), (False, 1)):
                l = 1 - l if stage == 1 else l
                sent[forward, stage, a].wait_recv()
                o = across if stage == 2 else chips - 1 if forward else 1
                if stage == 0:
                    pass_on(forward, 2, o, l, a)
                shared.append(share(o, l, a))
    for copy in shared:
        copy.wait_recv()
    for copy in (*shared, *sent.values(), *told):
        copy.wait_send()


def put_out(*refs):
    *refs, sems = refs
    n = len(refs) // 2
    copies = [pltpu.make_async_copy(a, b, sems.at[i]) for i, (a, b) in enumerate(zip(refs[:n], refs[n:]))]
    for copy in copies:
        copy.start()
    for copy in copies:
        copy.wait()


def solution(mesh):
    size = mesh.shape["dp"]

    def step(*arrays):
        terms, weights, m, v = (arrays[i : i + 3] for i in (0, 3, 6, 9))
        count = size * sum(one.size for one in m)
        in_vmem = [pltpu.VMEM(x.shape, x.dtype) for x in (*weights, *m, *v)]
        blocks = [(LAYERS, *one.shape[1:]) for one in m]
        dma = lambda n: pltpu.SemaphoreType.DMA((n,))
        units = 4 * LAYERS * KINDS
        out = pl.pallas_call(
            functools.partial(kernel, size, count),
            out_shape=in_vmem,
            in_specs=[pl.BlockSpec(memory_space=pltpu.HBM)] * 12,
            out_specs=[pl.BlockSpec(memory_space=pltpu.VMEM)] * 9,
            scratch_shapes=[
                *(pltpu.VMEM(b, jnp.bfloat16) for b in blocks),
                *(pltpu.VMEM(b, jnp.bfloat16) for b in blocks),
                *(pltpu.VMEM((2, *b), jnp.bfloat16) for b in blocks),
                pltpu.VMEM((size, 8, 128), jnp.float32),
                dma(units),
                dma(18),
                dma(units),
                dma(units),
                dma(18),
                dma(18),
                dma(size - 1),
                dma(size - 1),
            ],
            compiler_params=pltpu.CompilerParams(
                collective_id=0, has_side_effects=True, vmem_limit_bytes=16 << 20
            ),
            name="step",
        )(*(pltpu.with_memory_space_constraint(x, pltpu.HBM) for x in arrays))
        return pl.pallas_call(
            put_out,
            out_shape=[jax.ShapeDtypeStruct(x.shape, x.dtype) for x in out],
            in_specs=[pl.BlockSpec(memory_space=pltpu.VMEM)] * 9,
            out_specs=[pl.BlockSpec(memory_space=pltpu.HBM)] * 9,
            scratch_shapes=[dma(9)],
            compiler_params=pltpu.CompilerParams(vmem_limit_bytes=16 << 20),
            name="put_out",
        )(*(x for x in out))

    all_of, cut = P(None, None, None), P(None, "dp", None)
    return jax.shard_map(
        step,
        mesh=mesh,
        in_specs=(P(("rep", "dp"), None, None, None),) * 3 + (all_of,) * 3 + (cut,) * 6,
        out_specs=(P("rep", None, None),) * 3 + (P("rep", "dp", None),) * 6,
        check_vma=False,
    )
```

```python
import functools

import jax
import jax.numpy as jnp
from jax import lax
from jax.experimental import pallas as pl
from jax.experimental.pallas import tpu as pltpu
from jax.sharding import PartitionSpec as P

LAYERS = 2
KINDS = 3
MESH = pl.DeviceIdType.MESH


def strip(columns):
    return 16 if columns > 1024 else 48


def tile_sum(x):
    tiles = [x[r : r + 8, c : c + 128] for r in range(0, x.shape[0], 8) for c in range(0, x.shape[1], 128)]
    while len(tiles) > 1:
        tiles = [a + b for a, b in zip(tiles[::2], tiles[1::2])] + ([tiles[-1]] if len(tiles) % 2 else [])
    return tiles[0]


def cut(rows, columns):
    pieces = []
    for a in range(KINDS):
        small = strip(columns[a])
        heights = [small, rows[a] - small] if a == 0 else [rows[a]] if a < KINDS - 1 else [rows[a] - small, small]
        pieces += [(a, sum(heights[:i]), h) for i, h in enumerate(heights)]
    return pieces


def kernel(size, count, pieces, *refs):
    chips = size // 2
    take = iter(refs)
    some = lambda n: [next(take) for _ in range(n)]
    g_in, w_in, m_in, v_in = some(KINDS), some(KINDS), some(KINDS), some(KINDS)
    W, M, V = some(KINDS), some(KINDS), some(KINDS)
    old, hop, last = some(KINDS), some(KINDS), some(KINDS)
    squares, own_sem, load_sem, peer_send, peer_recv, link_send, link_recv, sq_send, sq_recv = some(9)

    me = lax.axis_index("dp")
    chip, core = me // 2, lax.rem(me, 2)
    at = lambda offset: lax.rem(chip + offset, chips)
    sibling = chip * 2 + 1 - core
    ahead, behind = at(1) * 2 + core, at(chips - 1) * 2 + core
    across = chips // 2
    offsets = (across, 1, chips - 1, 0)
    rows = [m.shape[1] for m in m_in]
    every = range(len(pieces))

    barrier = pltpu.get_barrier_semaphore()
    for step in range(1, size):
        pl.semaphore_signal(barrier, inc=1, device_id={"dp": lax.rem(me + step, size)}, device_id_type=MESH)

    def block(q, device, start=None, height=None):
        a, first, high = pieces[q]
        start, height = (first, high) if start is None else (start, height)
        return pl.ds(pl.multiple_of(device * rows[a] + start, 16), height)

    def part(q):
        return pl.ds(pieces[q][1], pieces[q][2])

    def unit(o, l, q):
        return (offsets.index(o) * LAYERS + l) * len(pieces) + q

    def mine(o):
        return at(o) * 2 + core

    def theirs(o):
        return at(o) * 2 + 1 - core

    own, given = {}, {}

    def fetch(o):
        for q in every:
            for l in range(LAYERS):
                a, here = pieces[q][0], block(q, mine(o))
                own[o, l, q] = pltpu.make_async_copy(g_in[a].at[0, l, here], W[a].at[l, here], own_sem.at[unit(o, l, q)])
                own[o, l, q].start()

    def give(o):
        for q in every:
            for l in range(LAYERS):
                a = pieces[q][0]
                given[o, l, q] = pltpu.make_async_remote_copy(
                    g_in[a].at[0, l, block(q, theirs(o))],
                    W[a].at[l, block(q, mine(o))],
                    peer_send.at[unit(o, l, q)],
                    peer_recv.at[unit(o, l, q)],
                    device_id={"dp": sibling},
                    device_id_type=MESH,
                )
                given[o, l, q].start()

    def each_strip(q, body, init):
        a, first, high = pieces[q]
        height = strip(g_in[a].shape[-1])
        if high == height:
            return body(first, height, init)
        return lax.fori_loop(
            0, high // height, lambda i, carry: body(pl.multiple_of(first + i * height, 16), height, carry), init
        )

    def add(o, l, q, more=()):
        own[o, l, q].wait()
        given[o, l, q].wait_recv()
        a = pieces[q][0]

        def body(start, height, carry):
            here = W[a].at[l, block(q, mine(o), start, height)]
            total = here[...].astype(jnp.float32) + W[a][l, block(q, theirs(o), start, height)].astype(jnp.float32)
            for other in more:
                total = total + other[pl.ds(start, height)].astype(jnp.float32)
            total = total.astype(jnp.bfloat16)
            here[...] = total
            if o == 0:
                total = total.astype(jnp.float32)
                carry = carry + tile_sum(total * total)
            return carry

        return each_strip(q, body, jnp.zeros((8, 128), jnp.float32) if o == 0 else 0)

    sent = {}

    def to_link(forward, stage, q, source, target):
        slot = ((0 if forward else 1) * 3 + stage) * len(pieces) + q
        sent[forward, stage, q] = pltpu.make_async_remote_copy(
            source,
            target,
            link_send.at[slot],
            link_recv.at[slot],
            device_id={"dp": ahead if forward else behind},
            device_id_type=MESH,
        )
        sent[forward, stage, q].start()

    fetch(across)
    pl.semaphore_wait(barrier, size - 1)
    give(across)
    for o in (1, chips - 1):
        fetch(o)
        give(o)
    for q in every:
        for forward, l in ((True, 0), (False, 1)):
            add(across, l, q)
            a = pieces[q][0]
            to_link(forward, 0, q, W[a].at[l, block(q, mine(across))], hop[a].at[l, part(q)])
    fetch(0)
    give(0)
    for q in every:
        for forward, l in ((True, 1), (False, 0)):
            o = 1 if forward else chips - 1
            add(o, l, q)
            a = pieces[q][0]
            to_link(forward, 1, q, W[a].at[l, block(q, mine(o))], last[a].at[0 if forward else 1, l, part(q)])
    loads = []
    for l in range(LAYERS):
        for a in range(KINDS):
            its = pl.ds(pl.multiple_of(me * rows[a], 16), rows[a])
            for n, (source, target) in enumerate(
                ((w_in[a].at[l, its], old[a].at[l]), (m_in[a].at[l], M[a].at[l]), (v_in[a].at[l], V[a].at[l]))
            ):
                loads.append(pltpu.make_async_copy(source, target, load_sem.at[(l * KINDS + a) * 3 + n]))
                loads[-1].start()
    for q in every:
        for forward, l in ((True, 0), (False, 1)):
            o = 1 if forward else chips - 1
            sent[forward, 0, q].wait_recv()
            a = pieces[q][0]
            add(o, l, q, (hop[a].at[l],))
            to_link(forward, 2, q, W[a].at[l, block(q, mine(o))], last[a].at[0 if forward else 1, l, part(q)])
    for copy in loads:
        copy.wait()
    total = jnp.zeros((8, 128), jnp.float32)
    for q in every:
        for l in range(LAYERS):
            sent[True, 2 - l, q].wait_recv()
            sent[False, 1 + l, q].wait_recv()
            a = pieces[q][0]
            total = total + add(0, l, q, (last[a].at[0, l], last[a].at[1, l]))
    for copy in (*given.values(), *sent.values()):
        copy.wait_send()

    squares[me] = total
    told = []
    for step in range(1, size):
        told.append(
            pltpu.make_async_remote_copy(
                squares.at[me],
                squares.at[me],
                sq_send.at[step - 1],
                sq_recv.at[step - 1],
                device_id={"dp": lax.rem(me + step, size)},
                device_id_type=MESH,
            )
        )
        told[-1].start()
    for copy in told:
        copy.wait_recv()
    everything = jnp.sum(jnp.sum(squares[...], axis=0), keepdims=True)
    factor = jnp.minimum(1.0, 0.5 * lax.rsqrt(everything / count + 1e-30))

    def update(l, q):
        a = pieces[q][0]

        def body(start, height, carry):
            here = W[a].at[l, block(q, me, start, height)]
            its = pl.ds(start, height)
            g = here[...].astype(jnp.float32) * factor
            w = old[a][l, its].astype(jnp.float32)
            m = 0.9 * M[a][l, its] + 0.1 * g
            v = 0.95 * V[a][l, its] + 0.05 * g * g
            M[a][l, its] = m
            V[a][l, its] = v
            here[...] = (w - 0.02 * (m * lax.rsqrt(v + 1e-8) + 0.1 * w)).astype(jnp.bfloat16)
            return carry

        each_strip(q, body, 0)

    shared = []

    def share(o, l, q):
        place = W[pieces[q][0]].at[l, block(q, mine(o))]
        u = unit(o, l, q)
        shared.append(
            pltpu.make_async_remote_copy(
                place, place, peer_send.at[u], peer_recv.at[u], device_id={"dp": sibling}, device_id_type=MESH
            )
        )
        shared[-1].start()

    def pass_on(forward, stage, o, l, q):
        place = W[pieces[q][0]].at[l, block(q, mine(o))]
        to_link(forward, stage, q, place, place)

    for q in every:
        for forward, l in ((True, 0), (False, 1)):
            update(l, q)
            pass_on(forward, 0, 0, l, q)
    for q in every:
        for forward, l in ((True, 1), (False, 0)):
            pass_on(forward, 1, 0, l, q)
            share(0, l, q)
    for stage in range(3):
        for q in every:
            for forward, l in ((True, 0), (False, 1)):
                l = 1 - l if stage == 1 else l
                sent[forward, stage, q].wait_recv()
                o = across if stage == 2 else chips - 1 if forward else 1
                if stage == 0:
                    pass_on(forward, 2, o, l, q)
                share(o, l, q)
    for copy in shared:
        copy.wait_recv()
    for copy in (*shared, *sent.values(), *told):
        copy.wait_send()


def put_out(*refs):
    *refs, sems = refs
    n = len(refs) // 2
    copies = [pltpu.make_async_copy(a, b, sems.at[i]) for i, (a, b) in enumerate(zip(refs[:n], refs[n:]))]
    for copy in copies:
        copy.start()
    for copy in copies:
        copy.wait()


def solution(mesh):
    size = mesh.shape["dp"]

    def step(*arrays):
        terms, weights, m, v = (arrays[i : i + 3] for i in (0, 3, 6, 9))
        count = size * sum(one.size for one in m)
        in_vmem = [pltpu.VMEM(x.shape, x.dtype) for x in (*weights, *m, *v)]
        blocks = [(LAYERS, *one.shape[1:]) for one in m]
        dma = lambda n: pltpu.SemaphoreType.DMA((n,))
        pieces = cut([one.shape[1] for one in m], [one.shape[2] for one in m])
        units, hops = 4 * LAYERS * len(pieces), 6 * len(pieces)
        out = pl.pallas_call(
            functools.partial(kernel, size, count, pieces),
            out_shape=in_vmem,
            in_specs=[pl.BlockSpec(memory_space=pltpu.HBM)] * 12,
            out_specs=[pl.BlockSpec(memory_space=pltpu.VMEM)] * 9,
            scratch_shapes=[
                *(pltpu.VMEM(b, jnp.bfloat16) for b in blocks),
                *(pltpu.VMEM(b, jnp.bfloat16) for b in blocks),
                *(pltpu.VMEM((2, *b), jnp.bfloat16) for b in blocks),
                pltpu.VMEM((size, 8, 128), jnp.float32),
                dma(units),
                dma(3 * LAYERS * KINDS),
                dma(units),
                dma(units),
                dma(hops),
                dma(hops),
                dma(size - 1),
                dma(size - 1),
            ],
            compiler_params=pltpu.CompilerParams(
                collective_id=0, has_side_effects=True, vmem_limit_bytes=16 << 20
            ),
            name="step",
        )(*(pltpu.with_memory_space_constraint(x, pltpu.HBM) for x in arrays))
        return pl.pallas_call(
            put_out,
            out_shape=[jax.ShapeDtypeStruct(x.shape, x.dtype) for x in out],
            in_specs=[pl.BlockSpec(memory_space=pltpu.VMEM)] * 9,
            out_specs=[pl.BlockSpec(memory_space=pltpu.HBM)] * 9,
            scratch_shapes=[dma(9)],
            compiler_params=pltpu.CompilerParams(vmem_limit_bytes=16 << 20),
            name="put_out",
        )(*(x for x in out))

    whole, cut_rows = P(None, None, None), P(None, "dp", None)
    return jax.shard_map(
        step,
        mesh=mesh,
        in_specs=(P(("rep", "dp"), None, None, None),) * 3 + (whole,) * 3 + (cut_rows,) * 6,
        out_specs=(P("rep", None, None),) * 3 + (P("rep", "dp", None),) * 6,
        check_vma=False,
    )
```

```python
import functools

import jax
import jax.numpy as jnp
from jax import lax
from jax.experimental import pallas as pl
from jax.experimental.pallas import tpu as pltpu
from jax.sharding import PartitionSpec as P

LAYERS = 2
KINDS = 3
MESH = pl.DeviceIdType.MESH


def strip(columns):
    return 16 if columns > 1024 else 48


def tile_sum(x):
    tiles = [x[r : r + 8, c : c + 128] for r in range(0, x.shape[0], 8) for c in range(0, x.shape[1], 128)]
    while len(tiles) > 1:
        tiles = [a + b for a, b in zip(tiles[::2], tiles[1::2])] + ([tiles[-1]] if len(tiles) % 2 else [])
    return tiles[0]


def cut(rows, columns):
    pieces = []
    for a in range(KINDS):
        small = strip(columns[a])
        heights = [small, rows[a] - small] if a == 0 else [rows[a]] if a < KINDS - 1 else [rows[a] - small, small]
        pieces += [(a, sum(heights[:i]), h) for i, h in enumerate(heights)]
    return pieces


def seat(size):
    chips = size // 2
    me = lax.axis_index("dp")
    chip, core = me // 2, lax.rem(me, 2)
    at = lambda offset: lax.rem(chip + offset, chips)
    return me, chip, core, at, chip * 2 + 1 - core, at(1) * 2 + core, at(chips - 1) * 2 + core


def remote(source, target, send, recv, device):
    return pltpu.make_async_remote_copy(source, target, send, recv, device_id={"dp": device}, device_id_type=MESH)


def kernel(size, count, pieces, *refs):
    chips = size // 2
    take = iter(refs)
    some = lambda n: [next(take) for _ in range(n)]
    g_in, w_in, m_in, v_in = some(KINDS), some(KINDS), some(KINDS), some(KINDS)
    W, M, V, (up, kept) = some(1), some(KINDS), some(KINDS), some(2)
    W += some(KINDS - 1)
    old, hop, last = some(KINDS), some(KINDS), some(KINDS)
    squares, own_sem, load_sem, peer_send, peer_recv, link_send, link_recv, next_send, next_recv, sq_send, sq_recv = some(11)

    me, chip, core, at, sibling, ahead, behind = seat(size)
    across = chips // 2
    offsets = (across, 1, chips - 1, 0)
    rows = [m.shape[1] for m in m_in]
    every = range(len(pieces))
    ways = ((True, 0), (False, 1))

    barrier = pltpu.get_barrier_semaphore()
    for step in range(1, size):
        pl.semaphore_signal(barrier, inc=1, device_id={"dp": lax.rem(me + step, size)}, device_id_type=MESH)

    def block(q, device, start=None, height=None):
        a, first, high = pieces[q]
        start, height = (first, high) if start is None else (start, height)
        return pl.ds(pl.multiple_of(device * rows[a] + start, 16), height)

    def part(q):
        return pl.ds(pieces[q][1], pieces[q][2])

    def unit(o, l, q):
        return (offsets.index(o) * LAYERS + l) * len(pieces) + q

    def mine(o):
        return at(o) * 2 + core

    def theirs(o):
        return at(o) * 2 + 1 - core

    own, given = {}, {}

    def fetch(o):
        for q in every:
            for l in range(LAYERS):
                a, here = pieces[q][0], block(q, mine(o))
                own[o, l, q] = pltpu.make_async_copy(g_in[a].at[0, l, here], W[a].at[l, here], own_sem.at[unit(o, l, q)])
                own[o, l, q].start()

    def give(o):
        for q in every:
            for l in range(LAYERS):
                a, u = pieces[q][0], unit(o, l, q)
                given[o, l, q] = remote(
                    g_in[a].at[0, l, block(q, theirs(o))],
                    W[a].at[l, block(q, mine(o))],
                    peer_send.at[u],
                    peer_recv.at[u],
                    sibling,
                )
                given[o, l, q].start()

    def each_strip(q, body, init):
        a, first, high = pieces[q]
        height = strip(g_in[a].shape[-1])
        if high == height:
            return body(first, height, init)
        return lax.fori_loop(
            0, high // height, lambda i, carry: body(pl.multiple_of(first + i * height, 16), height, carry), init
        )

    def add(o, l, q, more=()):
        own[o, l, q].wait()
        given[o, l, q].wait_recv()
        a = pieces[q][0]

        def body(start, height, carry):
            here = W[a].at[l, block(q, mine(o), start, height)]
            total = here[...].astype(jnp.float32) + W[a][l, block(q, theirs(o), start, height)].astype(jnp.float32)
            for other in more:
                total = total + other[pl.ds(start, height)].astype(jnp.float32)
            total = total.astype(jnp.bfloat16)
            here[...] = total
            if o == 0:
                total = total.astype(jnp.float32)
                carry = carry + tile_sum(total * total)
            return carry

        return each_strip(q, body, jnp.zeros((8, 128), jnp.float32) if o == 0 else 0)

    sent = {}

    def to_link(forward, stage, q, source, target):
        slot = ((0 if forward else 1) * 3 + stage) * len(pieces) + q
        sent[forward, stage, q] = remote(
            source, target, link_send.at[slot], link_recv.at[slot], ahead if forward else behind
        )
        sent[forward, stage, q].start()

    fetch(across)
    pl.semaphore_wait(barrier, size - 1)
    give(across)
    for o in (1, chips - 1):
        fetch(o)
        give(o)
    for q in every:
        for forward, l in ways:
            add(across, l, q)
            a = pieces[q][0]
            to_link(forward, 0, q, W[a].at[l, block(q, mine(across))], hop[a].at[l, part(q)])
    fetch(0)
    give(0)
    for q in every:
        for forward, l in ((True, 1), (False, 0)):
            o = 1 if forward else chips - 1
            add(o, l, q)
            a = pieces[q][0]
            to_link(forward, 1, q, W[a].at[l, block(q, mine(o))], last[a].at[0 if forward else 1, l, part(q)])
    loads = []
    for l in range(LAYERS):
        for a in range(KINDS):
            its = pl.ds(pl.multiple_of(me * rows[a], 16), rows[a])
            for n, (source, target) in enumerate(
                ((w_in[a].at[l, its], old[a].at[l]), (m_in[a].at[l], M[a].at[l]), (v_in[a].at[l], V[a].at[l]))
            ):
                loads.append(pltpu.make_async_copy(source, target, load_sem.at[(l * KINDS + a) * 3 + n]))
                loads[-1].start()
    for q in every:
        for forward, l in ways:
            o = 1 if forward else chips - 1
            sent[forward, 0, q].wait_recv()
            a = pieces[q][0]
            add(o, l, q, (hop[a].at[l],))
            to_link(forward, 2, q, W[a].at[l, block(q, mine(o))], last[a].at[0 if forward else 1, l, part(q)])
    for copy in loads:
        copy.wait()
    total = jnp.zeros((8, 128), jnp.float32)
    for q in every:
        for l in range(LAYERS):
            sent[True, 2 - l, q].wait_recv()
            sent[False, 1 + l, q].wait_recv()
            a = pieces[q][0]
            total = total + add(0, l, q, (last[a].at[0, l], last[a].at[1, l]))
    for copy in (*given.values(), *sent.values()):
        copy.wait_send()

    squares[me] = total
    told = []
    for step in range(1, size):
        told.append(
            remote(
                squares.at[me], squares.at[me], sq_send.at[step - 1], sq_recv.at[step - 1], lax.rem(me + step, size)
            )
        )
        told[-1].start()
    for copy in told:
        copy.wait_recv()
    everything = jnp.sum(jnp.sum(squares[...], axis=0), keepdims=True)
    factor = jnp.minimum(1.0, 0.5 * lax.rsqrt(everything / count + 1e-30))

    def update(l, q):
        a = pieces[q][0]

        def body(start, height, carry):
            its = pl.ds(start, height)
            here = W[a].at[l, block(q, me, start, height)]
            g = here[...].astype(jnp.float32) * factor
            w = old[a][l, its].astype(jnp.float32)
            m = 0.9 * M[a][l, its] + 0.1 * g
            v = 0.95 * V[a][l, its] + 0.05 * g * g
            M[a][l, its] = m
            V[a][l, its] = v
            to = here if a == 0 else up.at[l, chip, its] if a == 1 else kept.at[l, its]
            to[...] = (w - 0.02 * (m * lax.rsqrt(v + 1e-8) + 0.1 * w)).astype(jnp.bfloat16)
            return carry

        each_strip(q, body, 0)

    shared = []

    def share(o, l, q):
        place = W[pieces[q][0]].at[l, block(q, mine(o))]
        u = unit(o, l, q)
        shared.append(remote(place, place, peer_send.at[u], peer_recv.at[u], sibling))
        shared[-1].start()

    def pass_on(forward, stage, o, l, q):
        place = W[pieces[q][0]].at[l, block(q, mine(o))]
        to_link(forward, stage, q, place, place)

    now = [q for q in every if pieces[q][0] == 0]
    for q in now:
        for forward, l in ways:
            update(l, q)
            pass_on(forward, 0, 0, l, q)
    for q in now:
        for forward, l in ((True, 1), (False, 0)):
            pass_on(forward, 1, 0, l, q)
            share(0, l, q)
    for q in every:
        if q not in now:
            for l in range(LAYERS):
                update(l, q)

    later = {}
    soon = [q for q in every if pieces[q][0] == 1]
    for stage in range(3):
        for i, q in enumerate(soon):
            for forward, l in ways:
                l = 1 - l if stage == 1 else l
                o = 0 if stage < 2 else chips - 1 if forward else 1
                slot = ((0 if forward else 1) * 3 + stage) * len(soon) + i
                place = up.at[l, at(o), part(q)]
                later[forward, stage, q] = remote(
                    place, place, next_send.at[slot], next_recv.at[slot], ahead if forward else behind
                )

    for stage in range(3):
        for q in now:
            for forward, l in ways:
                l = 1 - l if stage == 1 else l
                sent[forward, stage, q].wait_recv()
                o = across if stage == 2 else chips - 1 if forward else 1
                if stage == 0:
                    pass_on(forward, 2, o, l, q)
                share(o, l, q)
        if stage == 0:

            @pl.when(core == 1)
            def _():
                for (_, which, _), copy in later.items():
                    if which < 2:
                        copy.start()

    for copy in shared:
        copy.wait_recv()
    for copy in (*shared, *told):
        copy.wait_send()
    for (_, _, q), copy in sent.items():
        if q in now:
            copy.wait_send()

    @pl.when(core == 1)
    def _():
        for q in soon:
            for forward, _ in ways:
                later[forward, 0, q].wait_recv()
                later[forward, 2, q].start()
        for (_, which, _), copy in later.items():
            if which > 0:
                copy.wait_recv()
        for copy in later.values():
            copy.wait_send()


def gather(size, pieces, after, up, kept, *refs):
    W, (ready, peer_send, peer_recv, link_send, link_recv) = (None, *refs[:2]), refs[2:]
    chips = size // 2
    me, chip, core, at, sibling, ahead, behind = seat(size)
    across = chips // 2
    offsets = (across, 1, chips - 1, 0)
    every = range(len(pieces))
    ways = ((True, 0), (False, 1))
    heights = (None, up.shape[2], kept.shape[1])

    barrier = pltpu.get_barrier_semaphore()
    for peer in (ahead, behind):
        pl.semaphore_signal(barrier, inc=1, device_id={"dp": peer}, device_id_type=MESH)

    @pl.when(core == 0)
    def _():
        pl.semaphore_signal(barrier, inc=1, device_id={"dp": sibling}, device_id_type=MESH)

    pl.semaphore_wait(barrier, 2 + core)

    @pl.when(core == 1)
    def _():
        pl.semaphore_signal(ready, inc=1, device_id={"dp": sibling}, device_id_type=MESH)

    def target(o, l, q):
        a, first, high = pieces[q]
        return W[a].at[l, pl.ds(pl.multiple_of((at(o) * 2 + core) * heights[a] + first, 16), high)]

    def held(o, l, q):
        a, first, high = pieces[q]
        return up.at[l, at(o), pl.ds(first, high)] if a == 1 else kept.at[l, pl.ds(first, high)]

    sent, shares = {}, {}
    for q in every:
        for stage in range(3):
            for forward, l in ways:
                l = 1 - l if stage == 1 else l
                o = 0 if stage < 2 else chips - 1 if forward else 1
                slot = ((0 if forward else 1) * 3 + stage) * len(pieces) + q
                sent[forward, stage, q] = remote(
                    held(o, l, q) if o == 0 else target(o, l, q),
                    target(o, l, q),
                    link_send.at[slot],
                    link_recv.at[slot],
                    ahead if forward else behind,
                )
        for o in offsets:
            for l in range(LAYERS):
                u = (offsets.index(o) * LAYERS + l) * len(pieces) + q
                for early in (False, True):
                    source = held(o, l, q) if o == 0 or early else target(o, l, q)
                    if not early or pieces[q][0] == 1:
                        shares[o, l, q, early] = remote(source, target(o, l, q), peer_send.at[u], peer_recv.at[u], sibling)

    first = [q for q in every if pieces[q][0] == 1]
    then = [q for q in every if pieces[q][0] == 2]

    @pl.when(core == 0)
    def _():
        for stage in range(2):
            for q in first:
                for forward, _ in ways:
                    sent[forward, stage, q].start()

    @pl.when(core == 1)
    def _():
        for stage in range(2):
            for q in then:
                for forward, _ in ways:
                    sent[forward, stage, q].start()

    def keep(o, a, blocks):
        height = strip(blocks.shape[-1])
        row = pl.multiple_of((at(o) * 2 + core) * heights[a], 16)

        def body(i, carry):
            start = pl.multiple_of(i * height, 16)
            for l in range(LAYERS):
                source = blocks.at[l, at(o), pl.ds(start, height)] if a == 1 else blocks.at[l, pl.ds(start, height)]
                W[a][l, pl.ds(row + start, height)] = source[...]
            return carry

        lax.fori_loop(0, heights[a] // height, body, 0)

    keep(0, 1, up)
    keep(0, 2, kept)

    @pl.when(core == 0)
    def _():
        for q in first:
            for forward, _ in ways:
                sent[forward, 0, q].wait_recv()
                sent[forward, 2, q].start()
        for stage in range(2):
            for q in then:
                for forward, _ in ways:
                    sent[forward, stage, q].start()
        for stage in (1, 2):
            for q in first:
                for forward, _ in ways:
                    sent[forward, stage, q].wait_recv()
        pl.semaphore_wait(ready, 1)
        for o in offsets:
            for l in range(LAYERS):
                for q in first:
                    shares[o, l, q, False].start()

    @pl.when(core == 1)
    def _():
        for o in offsets:
            for l in range(LAYERS):
                for q in first:
                    shares[o, l, q, True].start()
        for o in offsets[:-1]:
            keep(o, 1, up)

    for l in range(LAYERS):
        for q in then:
            shares[0, l, q, False].start()
    for stage in range(3):
        for q in then:
            for forward, l in ways:
                l = 1 - l if stage == 1 else l
                o = across if stage == 2 else chips - 1 if forward else 1
                sent[forward, stage, q].wait_recv()
                if stage == 0:
                    sent[forward, 2, q].start()
                shares[o, l, q, False].start()
    for (_, _, _, early), copy in shares.items():
        if not early:
            copy.wait_recv()
            copy.wait_send()
    for (_, _, q), copy in sent.items():
        if q in then:
            copy.wait_send()

    @pl.when(core == 0)
    def _():
        for (_, _, q), copy in sent.items():
            if q in first:
                copy.wait_send()


def put_out(marked, *refs):
    *refs, sems = refs
    n = (len(refs) - marked) // 2
    pairs = list(zip(refs[:n], refs[n:]))
    if marked:
        pairs.append((refs[1].at[0, pl.ds(0, 8), pl.ds(0, 128)], refs[-1]))
    copies = [pltpu.make_async_copy(a, b, sems.at[i]) for i, (a, b) in enumerate(pairs)]
    for copy in copies:
        copy.start()
    for copy in copies:
        copy.wait()


def solution(mesh):
    size = mesh.shape["dp"]

    def step(*arrays):
        terms, weights, m, v = (arrays[i : i + 3] for i in (0, 3, 6, 9))
        count = size * sum(one.size for one in m)
        vmem = lambda xs: [pltpu.VMEM(x.shape, x.dtype) for x in xs]
        blocks = [pltpu.VMEM((LAYERS, *one.shape[1:]), jnp.bfloat16) for one in m]
        pairs = [pltpu.VMEM((2, LAYERS, *one.shape[1:]), jnp.bfloat16) for one in m]
        dma = lambda n: pltpu.SemaphoreType.DMA((n,))
        in_hbm, in_vmem = pl.BlockSpec(memory_space=pltpu.HBM), pl.BlockSpec(memory_space=pltpu.VMEM)
        grant = 31 << 20

        def put(marked, *results):
            shapes = [jax.ShapeDtypeStruct(x.shape, x.dtype) for x in results]
            shapes += [jax.ShapeDtypeStruct((8, 128), jnp.float32)] * marked
            return pl.pallas_call(
                functools.partial(put_out, marked),
                out_shape=shapes,
                in_specs=[in_vmem] * len(results),
                out_specs=[in_hbm] * len(shapes),
                scratch_shapes=[dma(len(shapes))],
                compiler_params=pltpu.CompilerParams(vmem_limit_bytes=grant),
                name="put_out",
            )(*results)

        pieces = cut([one.shape[1] for one in m], [one.shape[2] for one in m])
        units, hops = 4 * LAYERS * len(pieces), 6 * len(pieces)
        soon = sum(a == 1 for a, _, _ in pieces)
        up_shape = pltpu.VMEM((LAYERS, size // 2, *m[1].shape[1:]), jnp.bfloat16)
        *done, up, kept = pl.pallas_call(
            functools.partial(kernel, size, count, pieces),
            out_shape=[*vmem(weights[:1]), *vmem(m), *vmem(v), up_shape, blocks[-1]],
            in_specs=[in_hbm] * 12,
            out_specs=[in_vmem] * 9,
            scratch_shapes=[
                *vmem(weights[1:]),
                *blocks,
                *blocks,
                *pairs,
                pltpu.VMEM((size, 8, 128), jnp.float32),
                dma(units),
                dma(3 * LAYERS * KINDS),
                dma(units),
                dma(units),
                dma(hops),
                dma(hops),
                dma(6 * soon),
                dma(6 * soon),
                dma(size - 1),
                dma(size - 1),
            ],
            compiler_params=pltpu.CompilerParams(collective_id=0, has_side_effects=True, vmem_limit_bytes=grant),
            name="step",
        )(*(pltpu.with_memory_space_constraint(x, pltpu.HBM) for x in arrays))
        gate, *moments, after = put(1, *done)
        ends = [piece for piece in pieces if piece[0] > 0]
        units, hops = 4 * LAYERS * len(ends), 6 * len(ends)
        rest = pl.pallas_call(
            functools.partial(gather, size, ends),
            out_shape=vmem(weights[1:]),
            in_specs=[in_hbm, in_vmem, in_vmem],
            out_specs=[in_vmem] * 2,
            scratch_shapes=[pltpu.SemaphoreType.REGULAR, dma(units), dma(units), dma(hops), dma(hops)],
            compiler_params=pltpu.CompilerParams(collective_id=1, has_side_effects=True, vmem_limit_bytes=grant),
            name="gather",
        )(after, up, kept)
        return (gate, *put(0, *rest), *moments)

    whole, cut_rows = P(None, None, None), P(None, "dp", None)
    return jax.shard_map(
        step,
        mesh=mesh,
        in_specs=(P(("rep", "dp"), None, None, None),) * 3 + (whole,) * 3 + (cut_rows,) * 6,
        out_specs=(P("rep", None, None),) * 3 + (P("rep", "dp", None),) * 6,
        check_vma=False,
    )
```

```python
import functools

import jax
import jax.numpy as jnp
from jax import lax
from jax.experimental import pallas as pl
from jax.experimental.pallas import tpu as pltpu
from jax.sharding import PartitionSpec as P

LAYERS = 2
KINDS = 3
STAGES = 3
MESH = pl.DeviceIdType.MESH


def strip(columns):
    return 16 if columns > 1024 else 48


def tile_sum(x):
    tiles = [x[r : r + 8, c : c + 128] for r in range(0, x.shape[0], 8) for c in range(0, x.shape[1], 128)]
    while len(tiles) > 1:
        tiles = [a + b for a, b in zip(tiles[::2], tiles[1::2])] + ([tiles[-1]] if len(tiles) % 2 else [])
    return tiles[0]


def cut(rows, columns):
    pieces = []
    for a in range(KINDS):
        small = strip(columns[a])
        heights = [small, rows[a] - small] if a == 0 else [rows[a]] if a < KINDS - 1 else [rows[a] - small, small]
        pieces += [(a, sum(heights[:i]), h) for i, h in enumerate(heights)]
    return pieces


def seat(size):
    chips = size // 2
    me = lax.axis_index("dp")
    chip, core = me // 2, lax.rem(me, 2)
    at = lambda offset: lax.rem(chip + offset, chips)
    return me, chip, core, at, chip * 2 + 1 - core, at(1) * 2 + core, at(chips - 1) * 2 + core


def remote(source, target, send, recv, device):
    return pltpu.make_async_remote_copy(source, target, send, recv, device_id={"dp": device}, device_id_type=MESH)


def kernel(size, count, pieces, *refs):
    chips = size // 2
    take = iter(refs)
    some = lambda n: [next(take) for _ in range(n)]
    g_in, w_in, m_in, v_in = some(KINDS), some(KINDS), some(KINDS), some(KINDS)
    W, M, V, kept, (early,) = some(1), some(KINDS), some(KINDS), some(KINDS - 1), some(1)
    W += some(KINDS - 1)
    old, hop, last = some(KINDS), some(KINDS), some(KINDS)
    squares, own_sem, load_sem, peer_send, peer_recv, link_send, link_recv, next_send, next_recv, sq_send, sq_recv = some(11)

    me, chip, core, at, sibling, ahead, behind = seat(size)
    across = chips // 2
    offsets = (across, 1, chips - 1, 0)
    rows = [m.shape[1] for m in m_in]
    every = range(len(pieces))
    ways = ((True, 0), (False, 1))

    barrier = pltpu.get_barrier_semaphore()
    for step in range(1, size):
        pl.semaphore_signal(barrier, inc=1, device_id={"dp": lax.rem(me + step, size)}, device_id_type=MESH)

    def block(q, device, start=None, height=None):
        a, first, high = pieces[q]
        start, height = (first, high) if start is None else (start, height)
        return pl.ds(pl.multiple_of(device * rows[a] + start, 16), height)

    def part(q):
        return pl.ds(pieces[q][1], pieces[q][2])

    def unit(o, l, q):
        return (offsets.index(o) * LAYERS + l) * len(pieces) + q

    def mine(o):
        return at(o) * 2 + core

    def theirs(o):
        return at(o) * 2 + 1 - core

    own, given = {}, {}

    def fetch(o):
        for q in every:
            for l in range(LAYERS):
                a, here = pieces[q][0], block(q, mine(o))
                own[o, l, q] = pltpu.make_async_copy(g_in[a].at[0, l, here], W[a].at[l, here], own_sem.at[unit(o, l, q)])
                own[o, l, q].start()

    def give(o):
        for q in every:
            for l in range(LAYERS):
                a, u = pieces[q][0], unit(o, l, q)
                given[o, l, q] = remote(
                    g_in[a].at[0, l, block(q, theirs(o))],
                    W[a].at[l, block(q, mine(o))],
                    peer_send.at[u],
                    peer_recv.at[u],
                    sibling,
                )
                given[o, l, q].start()

    def each_strip(q, body, init):
        a, first, high = pieces[q]
        height = strip(g_in[a].shape[-1])
        if high == height:
            return body(first, height, init)
        return lax.fori_loop(
            0, high // height, lambda i, carry: body(pl.multiple_of(first + i * height, 16), height, carry), init
        )

    def add(o, l, q, more=()):
        own[o, l, q].wait()
        given[o, l, q].wait_recv()
        a = pieces[q][0]

        def body(start, height, carry):
            here = W[a].at[l, block(q, mine(o), start, height)]
            total = here[...].astype(jnp.float32) + W[a][l, block(q, theirs(o), start, height)].astype(jnp.float32)
            for other in more:
                total = total + other[pl.ds(start, height)].astype(jnp.float32)
            total = total.astype(jnp.bfloat16)
            here[...] = total
            if o == 0:
                total = total.astype(jnp.float32)
                carry = carry + tile_sum(total * total)
            return carry

        return each_strip(q, body, jnp.zeros((8, 128), jnp.float32) if o == 0 else 0)

    sent = {}

    def to_link(forward, stage, q, source, target):
        slot = ((0 if forward else 1) * 3 + stage) * len(pieces) + q
        sent[forward, stage, q] = remote(
            source, target, link_send.at[slot], link_recv.at[slot], ahead if forward else behind
        )
        sent[forward, stage, q].start()

    fetch(across)
    pl.semaphore_wait(barrier, size - 1)
    give(across)
    for o in (1, chips - 1):
        fetch(o)
        give(o)
    for q in every:
        for forward, l in ways:
            add(across, l, q)
            a = pieces[q][0]
            to_link(forward, 0, q, W[a].at[l, block(q, mine(across))], hop[a].at[l, part(q)])
    fetch(0)
    give(0)
    for q in every:
        for forward, l in ((True, 1), (False, 0)):
            o = 1 if forward else chips - 1
            add(o, l, q)
            a = pieces[q][0]
            to_link(forward, 1, q, W[a].at[l, block(q, mine(o))], last[a].at[0 if forward else 1, l, part(q)])
    loads = []
    for l in range(LAYERS):
        for a in range(KINDS):
            its = pl.ds(pl.multiple_of(me * rows[a], 16), rows[a])
            for n, (source, target) in enumerate(
                ((w_in[a].at[l, its], old[a].at[l]), (m_in[a].at[l], M[a].at[l]), (v_in[a].at[l], V[a].at[l]))
            ):
                loads.append(pltpu.make_async_copy(source, target, load_sem.at[(l * KINDS + a) * 3 + n]))
                loads[-1].start()
    for q in every:
        for forward, l in ways:
            o = 1 if forward else chips - 1
            sent[forward, 0, q].wait_recv()
            a = pieces[q][0]
            add(o, l, q, (hop[a].at[l],))
            to_link(forward, 2, q, W[a].at[l, block(q, mine(o))], last[a].at[0 if forward else 1, l, part(q)])
    for copy in loads:
        copy.wait()
    total = jnp.zeros((8, 128), jnp.float32)
    for q in every:
        for l in range(LAYERS):
            sent[True, 2 - l, q].wait_recv()
            sent[False, 1 + l, q].wait_recv()
            a = pieces[q][0]
            total = total + add(0, l, q, (last[a].at[0, l], last[a].at[1, l]))
    for copy in (*given.values(), *sent.values()):
        copy.wait_send()

    squares[me] = total
    told = []
    for step in range(1, size):
        told.append(
            remote(
                squares.at[me], squares.at[me], sq_send.at[step - 1], sq_recv.at[step - 1], lax.rem(me + step, size)
            )
        )
        told[-1].start()
    for copy in told:
        copy.wait_recv()
    everything = jnp.sum(jnp.sum(squares[...], axis=0), keepdims=True)
    factor = jnp.minimum(1.0, 0.5 * lax.rsqrt(everything / count + 1e-30))

    def update(l, q):
        a = pieces[q][0]

        def body(start, height, carry):
            its = pl.ds(start, height)
            here = W[a].at[l, block(q, me, start, height)]
            g = here[...].astype(jnp.float32) * factor
            w = old[a][l, its].astype(jnp.float32)
            m = 0.9 * M[a][l, its] + 0.1 * g
            v = 0.95 * V[a][l, its] + 0.05 * g * g
            M[a][l, its] = m
            V[a][l, its] = v
            to = here if a == 0 else kept[a - 1].at[l, its]
            to[...] = (w - 0.02 * (m * lax.rsqrt(v + 1e-8) + 0.1 * w)).astype(jnp.bfloat16)
            return carry

        each_strip(q, body, 0)

    shared = []

    def share(o, l, q):
        place = W[pieces[q][0]].at[l, block(q, mine(o))]
        u = unit(o, l, q)
        shared.append(remote(place, place, peer_send.at[u], peer_recv.at[u], sibling))
        shared[-1].start()

    def pass_on(forward, stage, o, l, q):
        place = W[pieces[q][0]].at[l, block(q, mine(o))]
        to_link(forward, stage, q, place, place)

    now = [q for q in every if pieces[q][0] == 0]
    for q in now:
        for forward, l in ways:
            update(l, q)
            pass_on(forward, 0, 0, l, q)
    for q in now:
        for forward, l in ((True, 1), (False, 0)):
            pass_on(forward, 1, 0, l, q)
            share(0, l, q)
    for q in every:
        if q not in now:
            for l in range(LAYERS):
                update(l, q)

    later = {}
    soon = [q for q in every if pieces[q][0] == 1]
    for stage in range(3):
        for i, q in enumerate(soon):
            for forward, l in ways:
                l = 1 - l if stage == 1 else l
                o = 0 if stage < 2 else chips - 1 if forward else 1
                slot = ((0 if forward else 1) * 3 + stage) * len(soon) + i
                place = early.at[l, at(o), part(q)]
                later[forward, stage, q] = remote(
                    kept[0].at[l, part(q)] if o == 0 else place,
                    place,
                    next_send.at[slot],
                    next_recv.at[slot],
                    ahead if forward else behind,
                )

    for stage in range(3):
        for q in now:
            for forward, l in ways:
                l = 1 - l if stage == 1 else l
                sent[forward, stage, q].wait_recv()
                o = across if stage == 2 else chips - 1 if forward else 1
                if stage == 0:
                    pass_on(forward, 2, o, l, q)
                share(o, l, q)
        if stage == 0:

            @pl.when(core == 1)
            def _():
                for (_, which, _), copy in later.items():
                    if which < 2:
                        copy.start()

    for copy in shared:
        copy.wait_recv()
    for copy in (*shared, *told):
        copy.wait_send()
    for (_, _, q), copy in sent.items():
        if q in now:
            copy.wait_send()

    @pl.when(core == 1)
    def _():
        for q in soon:
            for forward, _ in ways:
                later[forward, 0, q].wait_recv()
                later[forward, 2, q].start()
        for (_, which, _), copy in later.items():
            if which > 0:
                copy.wait_recv()
        for copy in later.values():
            copy.wait_send()


def gather(size, pieces, done, more, ahead_of, after, *refs):
    take = iter(refs)
    some = lambda n: [next(take) for _ in range(n)]
    kept, early = some(2)
    (kept_next,) = some(1) if more else (None,)
    (W,) = some(1)
    (early_next,) = some(1) if more else (None,)
    ready, peer_send, peer_recv, link_send, link_recv = some(5)
    next_send, next_recv = some(2) if more else (None, None)

    chips = size // 2
    me, chip, core, at, sibling, ahead, behind = seat(size)
    across = chips // 2
    offsets = (across, 1, chips - 1, 0)
    ways = ((True, 0), (False, 1))
    rows = kept.shape[1]
    height = strip(kept.shape[-1])

    barrier = pltpu.get_barrier_semaphore()
    for peer in (ahead, behind):
        pl.semaphore_signal(barrier, inc=1, device_id={"dp": peer}, device_id_type=MESH)

    @pl.when(core == 0)
    def _():
        pl.semaphore_signal(barrier, inc=1, device_id={"dp": sibling}, device_id_type=MESH)

    pl.semaphore_wait(barrier, 2 + core)

    @pl.when(core == 1)
    def _():
        pl.semaphore_signal(ready, inc=1, device_id={"dp": sibling}, device_id_type=MESH)

    def row(o, start):
        return pl.multiple_of((at(o) * 2 + core) * rows + start, 16)

    def hop(forward, stage):
        l = 0 if forward == (stage != 1) else 1
        behind_it = chips - 1 if forward else 1
        return l, 0 if stage < 2 else behind_it, behind_it if stage < 2 else across

    sent, rest, later, shares = {}, {}, {}, {}
    for i, (first, high) in enumerate(pieces):
        for stage in range(3):
            for forward, _ in ways:
                l, o, _ = hop(forward, stage)
                slot = ((0 if forward else 1) * 3 + stage) * len(pieces) + i
                target = W.at[l, pl.ds(row(o, first), high)]
                its = link_send.at[slot], link_recv.at[slot], ahead if forward else behind
                sent[forward, stage, i] = remote(kept.at[l, pl.ds(first, high)] if o == 0 else target, target, *its)
                if stage >= done:
                    rest[forward, stage, i] = remote(early.at[l, at(o), pl.ds(first, high)], target, *its)
        for o in offsets:
            for l in range(LAYERS):
                u = (offsets.index(o) * LAYERS + l) * len(pieces) + i
                target = W.at[l, pl.ds(row(o, first), high)]
                held = early.at[l, at(o), pl.ds(first, high)]
                for one in range(2):
                    source = kept.at[l, pl.ds(first, high)] if o == 0 else held if one and (o != across or done == 3) else target
                    shares[one, o, l, i] = remote(source, target, peer_send.at[u], peer_recv.at[u], sibling)
    for i, (first, high) in enumerate(more):
        for stage in range(ahead_of):
            for forward, _ in ways:
                l, o, _ = hop(forward, stage)
                slot = ((0 if forward else 1) * 3 + stage) * len(more) + i
                target = early_next.at[l, at(o), pl.ds(first, high)]
                later[forward, stage, i] = remote(
                    kept_next.at[l, pl.ds(first, high)] if o == 0 else target,
                    target,
                    next_send.at[slot],
                    next_recv.at[slot],
                    ahead if forward else behind,
                )

    def keep(o):
        def body(n, carry):
            start = pl.multiple_of(n * height, 16)
            for l in range(LAYERS):
                source = kept.at[l, pl.ds(start, height)] if o == 0 else early.at[l, at(o), pl.ds(start, height)]
                W[l, pl.ds(row(o, start), height)] = source[...]
            return carry

        lax.fori_loop(0, rows // height, body, 0)

    each = range(len(pieces))

    @pl.when(core == 0)
    def _():
        for stage in range(2):
            for i in each:
                for forward, _ in ways:
                    sent[forward, stage, i].start()
        keep(0)
        for i in each:
            for forward, _ in ways:
                sent[forward, 0, i].wait_recv()
                sent[forward, 2, i].start()
        pl.semaphore_wait(ready, 1)
        for i in each:
            for l in range(LAYERS):
                shares[0, 0, l, i].start()
        for stage in range(3):
            for i in each:
                for forward, _ in ways:
                    l, _, o = hop(forward, stage)
                    if stage > 0:
                        sent[forward, stage, i].wait_recv()
                    shares[0, o, l, i].start()
        for copy in sent.values():
            copy.wait_send()

    @pl.when(core == 1)
    def _():
        for copy in rest.values():
            copy.start()
        for (_, stage, _), copy in later.items():
            if stage < 2:
                copy.start()
        here = [o for o in offsets if o != across or done == 3]
        for o in here:
            for i in each:
                for l in range(LAYERS):
                    shares[1, o, l, i].start()
        for o in here:
            keep(o)
        for (forward, stage, i), copy in rest.items():
            l, _, o = hop(forward, stage)
            copy.wait_recv()
            shares[1, o, l, i].start()
        for i in range(len(more)):
            for forward, _ in ways:
                later[forward, 0, i].wait_recv()
                if ahead_of == 3:
                    later[forward, 2, i].start()

    for (one, _, _, _), copy in shares.items():
        if one == 0:
            copy.wait_recv()
            copy.wait_send()

    @pl.when(core == 1)
    def _():
        for copy in rest.values():
            copy.wait_send()
        for (_, stage, _), copy in later.items():
            if stage > 0:
                copy.wait_recv()
        for copy in later.values():
            copy.wait_send()


def put_out(marked, *refs):
    *refs, sems = refs
    n = (len(refs) - marked) // 2
    pairs = list(zip(refs[:n], refs[n:]))
    if marked:
        pairs.append((refs[0].at[0, pl.ds(0, 16), pl.ds(0, 128)], refs[-1]))
    copies = [pltpu.make_async_copy(a, b, sems.at[i]) for i, (a, b) in enumerate(pairs)]
    for copy in copies:
        copy.start()
    for copy in copies:
        copy.wait()


def solution(mesh):
    size = mesh.shape["dp"]

    def step(*arrays):
        terms, weights, m, v = (arrays[i : i + 3] for i in (0, 3, 6, 9))
        count = size * sum(one.size for one in m)
        vmem = lambda xs: [pltpu.VMEM(x.shape, x.dtype) for x in xs]
        blocks = [pltpu.VMEM((LAYERS, *one.shape[1:]), jnp.bfloat16) for one in m]
        pairs = [pltpu.VMEM((2, LAYERS, *one.shape[1:]), jnp.bfloat16) for one in m]
        dma = lambda n: pltpu.SemaphoreType.DMA((n,))
        in_hbm, in_vmem = pl.BlockSpec(memory_space=pltpu.HBM), pl.BlockSpec(memory_space=pltpu.VMEM)
        grant = 31 << 20

        def put(marked, *results):
            shapes = [jax.ShapeDtypeStruct(x.shape, x.dtype) for x in results]
            shapes += [jax.ShapeDtypeStruct((16, 128), jnp.bfloat16)] * marked
            return pl.pallas_call(
                functools.partial(put_out, marked),
                out_shape=shapes,
                in_specs=[in_vmem] * len(results),
                out_specs=[in_hbm] * len(shapes),
                scratch_shapes=[dma(len(shapes))],
                compiler_params=pltpu.CompilerParams(vmem_limit_bytes=grant),
                name="put_out",
            )(*results)

        pieces = cut([one.shape[1] for one in m], [one.shape[2] for one in m])
        units, hops = 4 * LAYERS * len(pieces), 6 * len(pieces)
        soon = sum(a == 1 for a, _, _ in pieces)
        early = [pltpu.VMEM((LAYERS, size // 2, *one.shape[1:]), jnp.bfloat16) for one in m]
        *done, kept_up, kept_down, early_up = pl.pallas_call(
            functools.partial(kernel, size, count, pieces),
            out_shape=[*vmem(weights[:1]), *vmem(m), *vmem(v), *blocks[1:], early[1]],
            in_specs=[in_hbm] * 12,
            out_specs=[in_vmem] * 10,
            scratch_shapes=[
                *vmem(weights[1:]),
                *blocks,
                *blocks,
                *pairs,
                pltpu.VMEM((size, 8, 128), jnp.float32),
                dma(units),
                dma(3 * LAYERS * KINDS),
                dma(units),
                dma(units),
                dma(hops),
                dma(hops),
                dma(6 * soon),
                dma(6 * soon),
                dma(size - 1),
                dma(size - 1),
            ],
            compiler_params=pltpu.CompilerParams(collective_id=0, has_side_effects=True, vmem_limit_bytes=grant),
            name="step",
        )(*(pltpu.with_memory_space_constraint(x, pltpu.HBM) for x in arrays))
        gate, *moments, after = put(1, *done)
        ends = [[(first, high) for kind, first, high in pieces if kind == a] for a in range(KINDS)]

        def finish(a, done, ahead_of, *held):
            more = ends[a + 1] if ahead_of else []
            units, hops = 4 * LAYERS * len(ends[a]), 6 * len(ends[a])
            return pl.pallas_call(
                functools.partial(gather, size, ends[a], done, more, ahead_of),
                out_shape=[*vmem(weights[a : a + 1]), *(early[a + 1 : a + 2] if more else [])],
                in_specs=[in_hbm] + [in_vmem] * (len(held) - 1),
                out_specs=[in_vmem] * (2 if more else 1),
                scratch_shapes=[
                    pltpu.SemaphoreType.REGULAR,
                    dma(units),
                    dma(units),
                    dma(hops),
                    dma(hops),
                    *([dma(6 * len(more))] * 2 if more else []),
                ],
                compiler_params=pltpu.CompilerParams(collective_id=a, has_side_effects=True, vmem_limit_bytes=grant),
                name=f"gather_{a}",
            )(*held)

        up, early_down = finish(1, 3, STAGES, after, kept_up, early_up, kept_down)
        up, after = put(1, up)
        (down,) = finish(2, STAGES, 0, after, kept_down, early_down)
        (down,) = put(0, down)
        return (gate, up, down, *moments)

    whole, cut_rows = P(None, None, None), P(None, "dp", None)
    return jax.shard_map(
        step,
        mesh=mesh,
        in_specs=(P(("rep", "dp"), None, None, None),) * 3 + (whole,) * 3 + (cut_rows,) * 6,
        out_specs=(P("rep", None, None),) * 3 + (P("rep", "dp", None),) * 6,
        check_vma=False,
    )
```

```python
import functools

import jax
import jax.numpy as jnp
from jax import lax
from jax.experimental import pallas as pl
from jax.experimental.pallas import tpu as pltpu
from jax.sharding import PartitionSpec as P

LAYERS = 2
KINDS = 3
STAGES = 3
MESH = pl.DeviceIdType.MESH


def strip(columns):
    return 16 if columns > 1024 else 48


def tile_sum(x):
    tiles = [x[r : r + 8, c : c + 128] for r in range(0, x.shape[0], 8) for c in range(0, x.shape[1], 128)]
    while len(tiles) > 1:
        tiles = [a + b for a, b in zip(tiles[::2], tiles[1::2])] + ([tiles[-1]] if len(tiles) % 2 else [])
    return tiles[0]


def cut(rows, columns):
    pieces = []
    for a in range(KINDS):
        small = strip(columns[a])
        heights = [small, rows[a] - small] if a == 0 else [rows[a]] if a < KINDS - 1 else [rows[a] - small, small]
        pieces += [(a, sum(heights[:i]), h) for i, h in enumerate(heights)]
    return pieces


def seat(size):
    chips = size // 2
    me = lax.axis_index("dp")
    chip, core = me // 2, lax.rem(me, 2)
    at = lambda offset: lax.rem(chip + offset, chips)
    return me, chip, core, at, chip * 2 + 1 - core, at(1) * 2 + core, at(chips - 1) * 2 + core


def remote(source, target, send, recv, device):
    return pltpu.make_async_remote_copy(source, target, send, recv, device_id={"dp": device}, device_id_type=MESH)


def kernel(size, count, pieces, *refs):
    chips = size // 2
    take = iter(refs)
    some = lambda n: [next(take) for _ in range(n)]
    g_in, w_in, m_in, v_in = some(KINDS), some(KINDS), some(KINDS), some(KINDS)
    W, M, V, kept, (early,) = some(1), some(KINDS), some(KINDS), some(KINDS - 1), some(1)
    W += some(KINDS - 1)
    old, hop, last = some(KINDS), some(KINDS), some(KINDS)
    squares, own_sem, load_sem, peer_send, peer_recv, link_send, link_recv, next_send, next_recv, sq_send, sq_recv, met = some(12)

    me, chip, core, at, sibling, ahead, behind = seat(size)
    across = chips // 2
    offsets = (across, 1, chips - 1, 0)
    rows = [m.shape[1] for m in m_in]
    every = range(len(pieces))
    ways = ((True, 0), (False, 1))

    barrier = pltpu.get_barrier_semaphore()

    def block(q, device, start=None, height=None):
        a, first, high = pieces[q]
        start, height = (first, high) if start is None else (start, height)
        return pl.ds(pl.multiple_of(device * rows[a] + start, 16), height)

    def part(q):
        return pl.ds(pieces[q][1], pieces[q][2])

    def unit(o, l, q):
        return (offsets.index(o) * LAYERS + l) * len(pieces) + q

    def mine(o):
        return at(o) * 2 + core

    def theirs(o):
        return at(o) * 2 + 1 - core

    own, given = {}, {}

    def fetch(o):
        for q in every:
            for l in range(LAYERS):
                a, here = pieces[q][0], block(q, mine(o))
                own[o, l, q] = pltpu.make_async_copy(g_in[a].at[0, l, here], W[a].at[l, here], own_sem.at[unit(o, l, q)])
                own[o, l, q].start()

    def give(o):
        for q in every:
            for l in range(LAYERS):
                a, u = pieces[q][0], unit(o, l, q)
                given[o, l, q] = remote(
                    g_in[a].at[0, l, block(q, theirs(o))],
                    W[a].at[l, block(q, mine(o))],
                    peer_send.at[u],
                    peer_recv.at[u],
                    sibling,
                )
                given[o, l, q].start()

    def each_strip(q, body, init):
        a, first, high = pieces[q]
        height = strip(g_in[a].shape[-1])
        if high == height:
            return body(first, height, init)
        return lax.fori_loop(
            0, high // height, lambda i, carry: body(pl.multiple_of(first + i * height, 16), height, carry), init
        )

    def add(o, l, q, more=()):
        own[o, l, q].wait()
        given[o, l, q].wait_recv()
        a = pieces[q][0]

        def body(start, height, carry):
            here = W[a].at[l, block(q, mine(o), start, height)]
            total = here[...].astype(jnp.float32) + W[a][l, block(q, theirs(o), start, height)].astype(jnp.float32)
            for other in more:
                total = total + other[pl.ds(start, height)].astype(jnp.float32)
            total = total.astype(jnp.bfloat16)
            here[...] = total
            if o == 0:
                total = total.astype(jnp.float32)
                carry = carry + tile_sum(total * total)
            return carry

        return each_strip(q, body, jnp.zeros((8, 128), jnp.float32) if o == 0 else 0)

    sent = {}

    def to_link(forward, stage, q, source, target):
        slot = ((0 if forward else 1) * 3 + stage) * len(pieces) + q
        sent[forward, stage, q] = remote(
            source, target, link_send.at[slot], link_recv.at[slot], ahead if forward else behind
        )
        sent[forward, stage, q].start()

    @pl.when(core == 1)
    def _():
        pl.semaphore_signal(barrier, inc=1, device_id={"dp": sibling}, device_id_type=MESH)

    fetch(across)

    @pl.when(core == 0)
    def _():
        pl.semaphore_wait(barrier, 1)
        pl.semaphore_signal(met, inc=1, device_id={"dp": sibling}, device_id_type=MESH)

    @pl.when(core == 1)
    def _():
        pl.semaphore_wait(met, 1)
        for peer in (ahead, behind):
            pl.semaphore_signal(barrier, inc=1, device_id={"dp": peer}, device_id_type=MESH)

    give(across)

    def greeted():
        @pl.when(core == 1)
        def _():
            pl.semaphore_wait(barrier, 2)
            pl.semaphore_signal(met, inc=1, device_id={"dp": sibling}, device_id_type=MESH)

        @pl.when(core == 0)
        def _():
            pl.semaphore_wait(met, 1)

    for q in every:
        for _, l in ways:
            add(across, l, q)
        if q == 0:
            greeted()
        for forward, l in ways:
            a = pieces[q][0]
            to_link(forward, 0, q, W[a].at[l, block(q, mine(across))], hop[a].at[l, part(q)])
        if q == 0:
            for o in (1, chips - 1):
                fetch(o)
                give(o)
    fetch(0)
    give(0)
    for q in every:
        for forward, l in ((True, 1), (False, 0)):
            o = 1 if forward else chips - 1
            add(o, l, q)
            a = pieces[q][0]
            to_link(forward, 1, q, W[a].at[l, block(q, mine(o))], last[a].at[0 if forward else 1, l, part(q)])
    loads = []
    for l in range(LAYERS):
        for a in range(KINDS):
            its = pl.ds(pl.multiple_of(me * rows[a], 16), rows[a])
            for n, (source, target) in enumerate(
                ((w_in[a].at[l, its], old[a].at[l]), (m_in[a].at[l], M[a].at[l]), (v_in[a].at[l], V[a].at[l]))
            ):
                loads.append(pltpu.make_async_copy(source, target, load_sem.at[(l * KINDS + a) * 3 + n]))
                loads[-1].start()
    for q in every:
        for forward, l in ways:
            o = 1 if forward else chips - 1
            sent[forward, 0, q].wait_recv()
            a = pieces[q][0]
            add(o, l, q, (hop[a].at[l],))
            to_link(forward, 2, q, W[a].at[l, block(q, mine(o))], last[a].at[0 if forward else 1, l, part(q)])
    for copy in loads:
        copy.wait()
    total = jnp.zeros((8, 128), jnp.float32)
    for q in every:
        for l in range(LAYERS):
            sent[True, 2 - l, q].wait_recv()
            sent[False, 1 + l, q].wait_recv()
            a = pieces[q][0]
            total = total + add(0, l, q, (last[a].at[0, l], last[a].at[1, l]))
    for copy in (*given.values(), *sent.values()):
        copy.wait_send()

    squares[me] = total
    told = []
    for step in range(1, size):
        told.append(
            remote(
                squares.at[me], squares.at[me], sq_send.at[step - 1], sq_recv.at[step - 1], lax.rem(me + step, size)
            )
        )
        told[-1].start()
    for copy in told:
        copy.wait_recv()
    everything = jnp.sum(jnp.sum(squares[...], axis=0), keepdims=True)
    factor = jnp.minimum(1.0, 0.5 * lax.rsqrt(everything / count + 1e-30))

    def update(l, q):
        a = pieces[q][0]

        def body(start, height, carry):
            its = pl.ds(start, height)
            here = W[a].at[l, block(q, me, start, height)]
            g = here[...].astype(jnp.float32) * factor
            w = old[a][l, its].astype(jnp.float32)
            m = 0.9 * M[a][l, its] + 0.1 * g
            v = 0.95 * V[a][l, its] + 0.05 * g * g
            M[a][l, its] = m
            V[a][l, its] = v
            to = here if a == 0 else kept[a - 1].at[l, its]
            to[...] = (w - 0.02 * (m * lax.rsqrt(v + 1e-8) + 0.1 * w)).astype(jnp.bfloat16)
            return carry

        each_strip(q, body, 0)

    shared = []

    def share(o, l, q):
        place = W[pieces[q][0]].at[l, block(q, mine(o))]
        u = unit(o, l, q)
        shared.append(remote(place, place, peer_send.at[u], peer_recv.at[u], sibling))
        shared[-1].start()

    def pass_on(forward, stage, o, l, q):
        place = W[pieces[q][0]].at[l, block(q, mine(o))]
        to_link(forward, stage, q, place, place)

    now = [q for q in every if pieces[q][0] == 0]
    for q in now:
        for forward, l in ways:
            update(l, q)
            pass_on(forward, 0, 0, l, q)
    for q in now:
        for forward, l in ((True, 1), (False, 0)):
            pass_on(forward, 1, 0, l, q)
            share(0, l, q)
    for q in every:
        if q not in now:
            for l in range(LAYERS):
                update(l, q)

    later = {}
    soon = [q for q in every if pieces[q][0] == 1]
    for stage in range(3):
        for i, q in enumerate(soon):
            for forward, l in ways:
                l = 1 - l if stage == 1 else l
                o = 0 if stage < 2 else chips - 1 if forward else 1
                slot = ((0 if forward else 1) * 3 + stage) * len(soon) + i
                place = early.at[l, at(o), part(q)]
                later[forward, stage, q] = remote(
                    kept[0].at[l, part(q)] if o == 0 else place,
                    place,
                    next_send.at[slot],
                    next_recv.at[slot],
                    ahead if forward else behind,
                )

    for stage in range(3):
        for q in now:
            for forward, l in ways:
                l = 1 - l if stage == 1 else l
                sent[forward, stage, q].wait_recv()
                o = across if stage == 2 else chips - 1 if forward else 1
                if stage == 0:
                    pass_on(forward, 2, o, l, q)
                share(o, l, q)
        if stage == 0:

            @pl.when(core == 1)
            def _():
                for (_, which, _), copy in later.items():
                    if which < 2:
                        copy.start()

    for copy in shared:
        copy.wait_recv()
    for copy in (*shared, *told):
        copy.wait_send()
    for (_, _, q), copy in sent.items():
        if q in now:
            copy.wait_send()

    @pl.when(core == 1)
    def _():
        for q in soon:
            for forward, _ in ways:
                later[forward, 0, q].wait_recv()
                later[forward, 2, q].start()
        for (_, which, _), copy in later.items():
            if which > 0:
                copy.wait_recv()
        for copy in later.values():
            copy.wait_send()


def gather(size, pieces, done, more, ahead_of, after, *refs):
    take = iter(refs)
    some = lambda n: [next(take) for _ in range(n)]
    kept, early = some(2)
    (kept_next,) = some(1) if more else (None,)
    (W,) = some(1)
    (early_next,) = some(1) if more else (None,)
    ready, peer_send, peer_recv, link_send, link_recv = some(5)
    next_send, next_recv = some(2) if more else (None, None)

    chips = size // 2
    me, chip, core, at, sibling, ahead, behind = seat(size)
    across = chips // 2
    offsets = (across, 1, chips - 1, 0)
    ways = ((True, 0), (False, 1))
    rows = kept.shape[1]
    height = strip(kept.shape[-1])

    barrier = pltpu.get_barrier_semaphore()
    for peer in (ahead, behind):
        pl.semaphore_signal(barrier, inc=1, device_id={"dp": peer}, device_id_type=MESH)

    @pl.when(core == 0)
    def _():
        pl.semaphore_signal(barrier, inc=1, device_id={"dp": sibling}, device_id_type=MESH)

    pl.semaphore_wait(barrier, 2 + core)

    @pl.when(core == 1)
    def _():
        pl.semaphore_signal(ready, inc=1, device_id={"dp": sibling}, device_id_type=MESH)

    def row(o, start):
        return pl.multiple_of((at(o) * 2 + core) * rows + start, 16)

    def hop(forward, stage):
        l = 0 if forward == (stage != 1) else 1
        behind_it = chips - 1 if forward else 1
        return l, 0 if stage < 2 else behind_it, behind_it if stage < 2 else across

    sent, rest, later, shares = {}, {}, {}, {}
    for i, (first, high) in enumerate(pieces):
        for stage in range(3):
            for forward, _ in ways:
                l, o, _ = hop(forward, stage)
                slot = ((0 if forward else 1) * 3 + stage) * len(pieces) + i
                target = W.at[l, pl.ds(row(o, first), high)]
                its = link_send.at[slot], link_recv.at[slot], ahead if forward else behind
                sent[forward, stage, i] = remote(kept.at[l, pl.ds(first, high)] if o == 0 else target, target, *its)
                if stage >= done:
                    rest[forward, stage, i] = remote(early.at[l, at(o), pl.ds(first, high)], target, *its)
        for o in offsets:
            for l in range(LAYERS):
                u = (offsets.index(o) * LAYERS + l) * len(pieces) + i
                target = W.at[l, pl.ds(row(o, first), high)]
                held = early.at[l, at(o), pl.ds(first, high)]
                for one in range(2):
                    source = kept.at[l, pl.ds(first, high)] if o == 0 else held if one and (o != across or done == 3) else target
                    shares[one, o, l, i] = remote(source, target, peer_send.at[u], peer_recv.at[u], sibling)
    for i, (first, high) in enumerate(more):
        for stage in range(ahead_of):
            for forward, _ in ways:
                l, o, _ = hop(forward, stage)
                slot = ((0 if forward else 1) * 3 + stage) * len(more) + i
                target = early_next.at[l, at(o), pl.ds(first, high)]
                later[forward, stage, i] = remote(
                    kept_next.at[l, pl.ds(first, high)] if o == 0 else target,
                    target,
                    next_send.at[slot],
                    next_recv.at[slot],
                    ahead if forward else behind,
                )

    def keep(o):
        def body(n, carry):
            start = pl.multiple_of(n * height, 16)
            for l in range(LAYERS):
                source = kept.at[l, pl.ds(start, height)] if o == 0 else early.at[l, at(o), pl.ds(start, height)]
                W[l, pl.ds(row(o, start), height)] = source[...]
            return carry

        lax.fori_loop(0, rows // height, body, 0)

    each = range(len(pieces))

    @pl.when(core == 0)
    def _():
        for stage in range(2):
            for i in each:
                for forward, _ in ways:
                    sent[forward, stage, i].start()
        keep(0)
        for i in each:
            for forward, _ in ways:
                sent[forward, 0, i].wait_recv()
                sent[forward, 2, i].start()
        pl.semaphore_wait(ready, 1)
        for i in each:
            for l in range(LAYERS):
                shares[0, 0, l, i].start()
        for stage in range(3):
            for i in each:
                for forward, _ in ways:
                    l, _, o = hop(forward, stage)
                    if stage > 0:
                        sent[forward, stage, i].wait_recv()
                    shares[0, o, l, i].start()
        for copy in sent.values():
            copy.wait_send()

    @pl.when(core == 1)
    def _():
        for copy in rest.values():
            copy.start()
        for (_, stage, _), copy in later.items():
            if stage < 2:
                copy.start()
        here = [o for o in offsets if o != across or done == 3]
        for o in here:
            for i in each:
                for l in range(LAYERS):
                    shares[1, o, l, i].start()
        for o in here:
            keep(o)
        for (forward, stage, i), copy in rest.items():
            l, _, o = hop(forward, stage)
            copy.wait_recv()
            shares[1, o, l, i].start()
        for i in range(len(more)):
            for forward, _ in ways:
                later[forward, 0, i].wait_recv()
                if ahead_of == 3:
                    later[forward, 2, i].start()

    for (one, _, _, _), copy in shares.items():
        if one == 0:
            copy.wait_recv()
            copy.wait_send()

    @pl.when(core == 1)
    def _():
        for copy in rest.values():
            copy.wait_send()
        for (_, stage, _), copy in later.items():
            if stage > 0:
                copy.wait_recv()
        for copy in later.values():
            copy.wait_send()


def put_out(marked, *refs):
    *refs, sems = refs
    n = (len(refs) - marked) // 2
    pairs = list(zip(refs[:n], refs[n:]))
    if marked:
        pairs.append((refs[0].at[0, pl.ds(0, 16), pl.ds(0, 128)], refs[-1]))
    copies = [pltpu.make_async_copy(a, b, sems.at[i]) for i, (a, b) in enumerate(pairs)]
    for copy in copies:
        copy.start()
    for copy in copies:
        copy.wait()


def solution(mesh):
    size = mesh.shape["dp"]

    def step(*arrays):
        terms, weights, m, v = (arrays[i : i + 3] for i in (0, 3, 6, 9))
        count = size * sum(one.size for one in m)
        vmem = lambda xs: [pltpu.VMEM(x.shape, x.dtype) for x in xs]
        blocks = [pltpu.VMEM((LAYERS, *one.shape[1:]), jnp.bfloat16) for one in m]
        pairs = [pltpu.VMEM((2, LAYERS, *one.shape[1:]), jnp.bfloat16) for one in m]
        dma = lambda n: pltpu.SemaphoreType.DMA((n,))
        in_hbm, in_vmem = pl.BlockSpec(memory_space=pltpu.HBM), pl.BlockSpec(memory_space=pltpu.VMEM)
        grant = 31 << 20

        def put(marked, *results):
            shapes = [jax.ShapeDtypeStruct(x.shape, x.dtype) for x in results]
            shapes += [jax.ShapeDtypeStruct((16, 128), jnp.bfloat16)] * marked
            return pl.pallas_call(
                functools.partial(put_out, marked),
                out_shape=shapes,
                in_specs=[in_vmem] * len(results),
                out_specs=[in_hbm] * len(shapes),
                scratch_shapes=[dma(len(shapes))],
                compiler_params=pltpu.CompilerParams(vmem_limit_bytes=grant),
                name="put_out",
            )(*results)

        pieces = cut([one.shape[1] for one in m], [one.shape[2] for one in m])
        units, hops = 4 * LAYERS * len(pieces), 6 * len(pieces)
        soon = sum(a == 1 for a, _, _ in pieces)
        early = [pltpu.VMEM((LAYERS, size // 2, *one.shape[1:]), jnp.bfloat16) for one in m]
        *done, kept_up, kept_down, early_up = pl.pallas_call(
            functools.partial(kernel, size, count, pieces),
            out_shape=[*vmem(weights[:1]), *vmem(m), *vmem(v), *blocks[1:], early[1]],
            in_specs=[in_hbm] * 12,
            out_specs=[in_vmem] * 10,
            scratch_shapes=[
                *vmem(weights[1:]),
                *blocks,
                *blocks,
                *pairs,
                pltpu.VMEM((size, 8, 128), jnp.float32),
                dma(units),
                dma(3 * LAYERS * KINDS),
                dma(units),
                dma(units),
                dma(hops),
                dma(hops),
                dma(6 * soon),
                dma(6 * soon),
                dma(size - 1),
                dma(size - 1),
                pltpu.SemaphoreType.REGULAR,
            ],
            compiler_params=pltpu.CompilerParams(collective_id=0, has_side_effects=True, vmem_limit_bytes=grant),
            name="step",
        )(*(pltpu.with_memory_space_constraint(x, pltpu.HBM) for x in arrays))
        gate, *moments, after = put(1, *done)
        ends = [[(first, high) for kind, first, high in pieces if kind == a] for a in range(KINDS)]

        def finish(a, done, ahead_of, *held):
            more = ends[a + 1] if ahead_of else []
            units, hops = 4 * LAYERS * len(ends[a]), 6 * len(ends[a])
            return pl.pallas_call(
                functools.partial(gather, size, ends[a], done, more, ahead_of),
                out_shape=[*vmem(weights[a : a + 1]), *(early[a + 1 : a + 2] if more else [])],
                in_specs=[in_hbm] + [in_vmem] * (len(held) - 1),
                out_specs=[in_vmem] * (2 if more else 1),
                scratch_shapes=[
                    pltpu.SemaphoreType.REGULAR,
                    dma(units),
                    dma(units),
                    dma(hops),
                    dma(hops),
                    *([dma(6 * len(more))] * 2 if more else []),
                ],
                compiler_params=pltpu.CompilerParams(collective_id=a, has_side_effects=True, vmem_limit_bytes=grant),
                name=f"gather_{a}",
            )(*held)

        up, early_down = finish(1, 3, STAGES, after, kept_up, early_up, kept_down)
        up, after = put(1, up)
        (down,) = finish(2, STAGES, 0, after, kept_down, early_down)
        (down,) = put(0, down)
        return (gate, up, down, *moments)

    whole, cut_rows = P(None, None, None), P(None, "dp", None)
    return jax.shard_map(
        step,
        mesh=mesh,
        in_specs=(P(("rep", "dp"), None, None, None),) * 3 + (whole,) * 3 + (cut_rows,) * 6,
        out_specs=(P("rep", None, None),) * 3 + (P("rep", "dp", None),) * 6,
        check_vma=False,
    )
```

```python
import functools

import jax
import jax.numpy as jnp
from jax import lax
from jax.experimental import pallas as pl
from jax.experimental.pallas import tpu as pltpu
from jax.sharding import PartitionSpec as P

LAYERS = 2
KINDS = 3
STAGES = 3
MESH = pl.DeviceIdType.MESH


def strip(columns):
    return 16 if columns > 1024 else 48


def tile_sum(x):
    tiles = [x[r : r + 8, c : c + 128] for r in range(0, x.shape[0], 8) for c in range(0, x.shape[1], 128)]
    while len(tiles) > 1:
        tiles = [a + b for a, b in zip(tiles[::2], tiles[1::2])] + ([tiles[-1]] if len(tiles) % 2 else [])
    return tiles[0]


def cut(rows, columns):
    pieces = []
    for a in range(KINDS):
        small = strip(columns[a])
        heights = [small, 3 * small, rows[a] - 5 * small, small] if a == 0 else [rows[a]] if a < KINDS - 1 else [rows[a] - small, small]
        pieces += [(a, sum(heights[:i]), h) for i, h in enumerate(heights)]
    return pieces


def seat(size):
    chips = size // 2
    me = lax.axis_index("dp")
    chip, core = me // 2, lax.rem(me, 2)
    at = lambda offset: lax.rem(chip + offset, chips)
    return me, chip, core, at, chip * 2 + 1 - core, at(1) * 2 + core, at(chips - 1) * 2 + core


def remote(source, target, send, recv, device):
    return pltpu.make_async_remote_copy(source, target, send, recv, device_id={"dp": device}, device_id_type=MESH)


def kernel(size, count, pieces, *refs):
    chips = size // 2
    take = iter(refs)
    some = lambda n: [next(take) for _ in range(n)]
    g_in, w_in, m_in, v_in = some(KINDS), some(KINDS), some(KINDS), some(KINDS)
    W, M, V, kept, (early,) = some(1), some(KINDS), some(KINDS), some(KINDS - 1), some(1)
    W += some(KINDS - 1)
    old, hop, last = some(KINDS), some(KINDS), some(KINDS)
    squares, own_sem, load_sem, peer_send, peer_recv, link_send, link_recv, next_send, next_recv, sq_send, sq_recv, met = some(12)

    me, chip, core, at, sibling, ahead, behind = seat(size)
    across = chips // 2
    offsets = (across, 1, chips - 1, 0)
    rows = [m.shape[1] for m in m_in]
    every = range(len(pieces))
    ways = ((True, 0), (False, 1))

    barrier = pltpu.get_barrier_semaphore()

    def block(q, device, start=None, height=None):
        a, first, high = pieces[q]
        start, height = (first, high) if start is None else (start, height)
        return pl.ds(pl.multiple_of(device * rows[a] + start, 16), height)

    def part(q):
        return pl.ds(pieces[q][1], pieces[q][2])

    def unit(o, l, q):
        return (offsets.index(o) * LAYERS + l) * len(pieces) + q

    def mine(o):
        return at(o) * 2 + core

    def theirs(o):
        return at(o) * 2 + 1 - core

    own, given = {}, {}

    def fetch(o):
        for q in every:
            for l in range(LAYERS):
                a, here = pieces[q][0], block(q, mine(o))
                own[o, l, q] = pltpu.make_async_copy(g_in[a].at[0, l, here], W[a].at[l, here], own_sem.at[unit(o, l, q)])
                own[o, l, q].start()

    def give(o):
        for q in every:
            for l in range(LAYERS):
                a, u = pieces[q][0], unit(o, l, q)
                given[o, l, q] = remote(
                    g_in[a].at[0, l, block(q, theirs(o))],
                    W[a].at[l, block(q, mine(o))],
                    peer_send.at[u],
                    peer_recv.at[u],
                    sibling,
                )
                given[o, l, q].start()

    def each_strip(q, body, init):
        a, first, high = pieces[q]
        height = strip(g_in[a].shape[-1])
        if high == height:
            return body(first, height, init)
        return lax.fori_loop(
            0, high // height, lambda i, carry: body(pl.multiple_of(first + i * height, 16), height, carry), init
        )

    def add(o, l, q, more=()):
        own[o, l, q].wait()
        given[o, l, q].wait_recv()
        a = pieces[q][0]

        def body(start, height, carry):
            here = W[a].at[l, block(q, mine(o), start, height)]
            total = here[...].astype(jnp.float32) + W[a][l, block(q, theirs(o), start, height)].astype(jnp.float32)
            for other in more:
                total = total + other[pl.ds(start, height)].astype(jnp.float32)
            total = total.astype(jnp.bfloat16)
            here[...] = total
            if o == 0:
                total = total.astype(jnp.float32)
                carry = carry + tile_sum(total * total)
            return carry

        return each_strip(q, body, jnp.zeros((8, 128), jnp.float32) if o == 0 else 0)

    sent = {}

    def to_link(forward, stage, q, source, target):
        slot = ((0 if forward else 1) * 3 + stage) * len(pieces) + q
        sent[forward, stage, q] = remote(
            source, target, link_send.at[slot], link_recv.at[slot], ahead if forward else behind
        )
        sent[forward, stage, q].start()

    @pl.when(core == 1)
    def _():
        pl.semaphore_signal(barrier, inc=1, device_id={"dp": sibling}, device_id_type=MESH)

    fetch(across)

    @pl.when(core == 0)
    def _():
        pl.semaphore_wait(barrier, 1)
        pl.semaphore_signal(met, inc=1, device_id={"dp": sibling}, device_id_type=MESH)

    @pl.when(core == 1)
    def _():
        pl.semaphore_wait(met, 1)
        for peer in (ahead, behind):
            pl.semaphore_signal(barrier, inc=1, device_id={"dp": peer}, device_id_type=MESH)

    give(across)

    def greeted():
        @pl.when(core == 1)
        def _():
            pl.semaphore_wait(barrier, 2)
            pl.semaphore_signal(met, inc=1, device_id={"dp": sibling}, device_id_type=MESH)

        @pl.when(core == 0)
        def _():
            pl.semaphore_wait(met, 1)

    for q in every:
        for _, l in ways:
            add(across, l, q)
        if q == 0:
            greeted()
        for forward, l in ways:
            a = pieces[q][0]
            to_link(forward, 0, q, W[a].at[l, block(q, mine(across))], hop[a].at[l, part(q)])
        if q == 0:
            for o in (1, chips - 1):
                fetch(o)
                give(o)
    fetch(0)
    give(0)
    for q in every:
        for forward, l in ((True, 1), (False, 0)):
            o = 1 if forward else chips - 1
            add(o, l, q)
            a = pieces[q][0]
            to_link(forward, 1, q, W[a].at[l, block(q, mine(o))], last[a].at[0 if forward else 1, l, part(q)])
    loads = []
    for l in range(LAYERS):
        for a in range(KINDS):
            its = pl.ds(pl.multiple_of(me * rows[a], 16), rows[a])
            for n, (source, target) in enumerate(
                ((w_in[a].at[l, its], old[a].at[l]), (m_in[a].at[l], M[a].at[l]), (v_in[a].at[l], V[a].at[l]))
            ):
                loads.append(pltpu.make_async_copy(source, target, load_sem.at[(l * KINDS + a) * 3 + n]))
                loads[-1].start()
    for q in every:
        for forward, l in ways:
            o = 1 if forward else chips - 1
            sent[forward, 0, q].wait_recv()
            a = pieces[q][0]
            add(o, l, q, (hop[a].at[l],))
            to_link(forward, 2, q, W[a].at[l, block(q, mine(o))], last[a].at[0 if forward else 1, l, part(q)])
    for copy in loads:
        copy.wait()
    total = jnp.zeros((8, 128), jnp.float32)
    for q in every:
        for l in range(LAYERS):
            sent[True, 2 - l, q].wait_recv()
            sent[False, 1 + l, q].wait_recv()
            a = pieces[q][0]
            total = total + add(0, l, q, (last[a].at[0, l], last[a].at[1, l]))
    for copy in (*given.values(), *sent.values()):
        copy.wait_send()

    squares[me] = total
    told = []
    for step in range(1, size):
        told.append(
            remote(
                squares.at[me], squares.at[me], sq_send.at[step - 1], sq_recv.at[step - 1], lax.rem(me + step, size)
            )
        )
        told[-1].start()
    for copy in told:
        copy.wait_recv()
    everything = jnp.sum(jnp.sum(squares[...], axis=0), keepdims=True)
    factor = jnp.minimum(1.0, 0.5 * lax.rsqrt(everything / count + 1e-30))

    def update(l, q):
        a = pieces[q][0]

        def body(start, height, carry):
            its = pl.ds(start, height)
            here = W[a].at[l, block(q, me, start, height)]
            g = here[...].astype(jnp.float32) * factor
            w = old[a][l, its].astype(jnp.float32)
            m = 0.9 * M[a][l, its] + 0.1 * g
            v = 0.95 * V[a][l, its] + 0.05 * g * g
            M[a][l, its] = m
            V[a][l, its] = v
            to = here if a == 0 else kept[a - 1].at[l, its]
            to[...] = (w - 0.02 * (m * lax.rsqrt(v + 1e-8) + 0.1 * w)).astype(jnp.bfloat16)
            return carry

        each_strip(q, body, 0)

    shared = []

    def share(o, l, q):
        place = W[pieces[q][0]].at[l, block(q, mine(o))]
        u = unit(o, l, q)
        shared.append(remote(place, place, peer_send.at[u], peer_recv.at[u], sibling))
        shared[-1].start()

    def pass_on(forward, stage, o, l, q):
        place = W[pieces[q][0]].at[l, block(q, mine(o))]
        to_link(forward, stage, q, place, place)

    now = [q for q in every if pieces[q][0] == 0]
    for q in now:
        for forward, l in ways:
            update(l, q)
            pass_on(forward, 0, 0, l, q)
    for q in now:
        for forward, l in ((True, 1), (False, 0)):
            pass_on(forward, 1, 0, l, q)
            share(0, l, q)
    for q in every:
        if q not in now:
            for l in range(LAYERS):
                update(l, q)

    later = {}
    soon = [q for q in every if pieces[q][0] == 1]
    for stage in range(3):
        for i, q in enumerate(soon):
            for forward, l in ways:
                l = 1 - l if stage == 1 else l
                o = 0 if stage < 2 else chips - 1 if forward else 1
                slot = ((0 if forward else 1) * 3 + stage) * len(soon) + i
                place = early.at[l, at(o), part(q)]
                later[forward, stage, q] = remote(
                    kept[0].at[l, part(q)] if o == 0 else place,
                    place,
                    next_send.at[slot],
                    next_recv.at[slot],
                    ahead if forward else behind,
                )

    for stage in range(3):
        for q in now:
            for forward, l in ways:
                l = 1 - l if stage == 1 else l
                sent[forward, stage, q].wait_recv()
                o = across if stage == 2 else chips - 1 if forward else 1
                if stage == 0:
                    pass_on(forward, 2, o, l, q)
                share(o, l, q)
        if stage == 0:

            @pl.when(core == 1)
            def _():
                for (_, which, _), copy in later.items():
                    if which < 2:
                        copy.start()

    for copy in shared:
        copy.wait_recv()
    for copy in (*shared, *told):
        copy.wait_send()
    for (_, _, q), copy in sent.items():
        if q in now:
            copy.wait_send()

    @pl.when(core == 1)
    def _():
        for q in soon:
            for forward, _ in ways:
                later[forward, 0, q].wait_recv()
                later[forward, 2, q].start()
        for (_, which, _), copy in later.items():
            if which > 0:
                copy.wait_recv()
        for copy in later.values():
            copy.wait_send()


def gather(size, pieces, done, more, ahead_of, after, *refs):
    take = iter(refs)
    some = lambda n: [next(take) for _ in range(n)]
    kept, early = some(2)
    (kept_next,) = some(1) if more else (None,)
    (W,) = some(1)
    (early_next,) = some(1) if more else (None,)
    ready, peer_send, peer_recv, link_send, link_recv = some(5)
    next_send, next_recv = some(2) if more else (None, None)

    chips = size // 2
    me, chip, core, at, sibling, ahead, behind = seat(size)
    across = chips // 2
    offsets = (across, 1, chips - 1, 0)
    ways = ((True, 0), (False, 1))
    rows = kept.shape[1]
    height = strip(kept.shape[-1])

    barrier = pltpu.get_barrier_semaphore()
    for peer in (ahead, behind):
        pl.semaphore_signal(barrier, inc=1, device_id={"dp": peer}, device_id_type=MESH)

    @pl.when(core == 0)
    def _():
        pl.semaphore_signal(barrier, inc=1, device_id={"dp": sibling}, device_id_type=MESH)

    pl.semaphore_wait(barrier, 2 + core)

    @pl.when(core == 1)
    def _():
        pl.semaphore_signal(ready, inc=1, device_id={"dp": sibling}, device_id_type=MESH)

    def row(o, start):
        return pl.multiple_of((at(o) * 2 + core) * rows + start, 16)

    def hop(forward, stage):
        l = 0 if forward == (stage != 1) else 1
        behind_it = chips - 1 if forward else 1
        return l, 0 if stage < 2 else behind_it, behind_it if stage < 2 else across

    sent, rest, later, shares = {}, {}, {}, {}
    for i, (first, high) in enumerate(pieces):
        for stage in range(3):
            for forward, _ in ways:
                l, o, _ = hop(forward, stage)
                slot = ((0 if forward else 1) * 3 + stage) * len(pieces) + i
                target = W.at[l, pl.ds(row(o, first), high)]
                its = link_send.at[slot], link_recv.at[slot], ahead if forward else behind
                sent[forward, stage, i] = remote(kept.at[l, pl.ds(first, high)] if o == 0 else target, target, *its)
                if stage >= done:
                    rest[forward, stage, i] = remote(early.at[l, at(o), pl.ds(first, high)], target, *its)
        for o in offsets:
            for l in range(LAYERS):
                u = (offsets.index(o) * LAYERS + l) * len(pieces) + i
                target = W.at[l, pl.ds(row(o, first), high)]
                held = early.at[l, at(o), pl.ds(first, high)]
                for one in range(2):
                    source = kept.at[l, pl.ds(first, high)] if o == 0 else held if one and (o != across or done == 3) else target
                    shares[one, o, l, i] = remote(source, target, peer_send.at[u], peer_recv.at[u], sibling)
    for i, (first, high) in enumerate(more):
        for stage in range(ahead_of):
            for forward, _ in ways:
                l, o, _ = hop(forward, stage)
                slot = ((0 if forward else 1) * 3 + stage) * len(more) + i
                target = early_next.at[l, at(o), pl.ds(first, high)]
                later[forward, stage, i] = remote(
                    kept_next.at[l, pl.ds(first, high)] if o == 0 else target,
                    target,
                    next_send.at[slot],
                    next_recv.at[slot],
                    ahead if forward else behind,
                )

    def keep(o):
        def body(n, carry):
            start = pl.multiple_of(n * height, 16)
            for l in range(LAYERS):
                source = kept.at[l, pl.ds(start, height)] if o == 0 else early.at[l, at(o), pl.ds(start, height)]
                W[l, pl.ds(row(o, start), height)] = source[...]
            return carry

        lax.fori_loop(0, rows // height, body, 0)

    each = range(len(pieces))

    @pl.when(core == 0)
    def _():
        for stage in range(2):
            for i in each:
                for forward, _ in ways:
                    sent[forward, stage, i].start()
        keep(0)
        for i in each:
            for forward, _ in ways:
                sent[forward, 0, i].wait_recv()
                sent[forward, 2, i].start()
        pl.semaphore_wait(ready, 1)
        for i in each:
            for l in range(LAYERS):
                shares[0, 0, l, i].start()
        for stage in range(3):
            for i in each:
                for forward, _ in ways:
                    l, _, o = hop(forward, stage)
                    if stage > 0:
                        sent[forward, stage, i].wait_recv()
                    shares[0, o, l, i].start()
        for copy in sent.values():
            copy.wait_send()

    @pl.when(core == 1)
    def _():
        for copy in rest.values():
            copy.start()
        for (_, stage, _), copy in later.items():
            if stage < 2:
                copy.start()
        here = [o for o in offsets if o != across or done == 3]
        for o in here:
            for i in each:
                for l in range(LAYERS):
                    shares[1, o, l, i].start()
        for o in here:
            keep(o)
        for (forward, stage, i), copy in rest.items():
            l, _, o = hop(forward, stage)
            copy.wait_recv()
            shares[1, o, l, i].start()
        for i in range(len(more)):
            for forward, _ in ways:
                later[forward, 0, i].wait_recv()
                if ahead_of == 3:
                    later[forward, 2, i].start()

    for (one, _, _, _), copy in shares.items():
        if one == 0:
            copy.wait_recv()
            copy.wait_send()

    @pl.when(core == 1)
    def _():
        for copy in rest.values():
            copy.wait_send()
        for (_, stage, _), copy in later.items():
            if stage > 0:
                copy.wait_recv()
        for copy in later.values():
            copy.wait_send()


def put_out(marked, *refs):
    *refs, sems = refs
    n = (len(refs) - marked) // 2
    pairs = list(zip(refs[:n], refs[n:]))
    if marked:
        pairs.append((refs[0].at[0, pl.ds(0, 16), pl.ds(0, 128)], refs[-1]))
    copies = [pltpu.make_async_copy(a, b, sems.at[i]) for i, (a, b) in enumerate(pairs)]
    for copy in copies:
        copy.start()
    for copy in copies:
        copy.wait()


def solution(mesh):
    size = mesh.shape["dp"]

    def step(*arrays):
        terms, weights, m, v = (arrays[i : i + 3] for i in (0, 3, 6, 9))
        count = size * sum(one.size for one in m)
        vmem = lambda xs: [pltpu.VMEM(x.shape, x.dtype) for x in xs]
        blocks = [pltpu.VMEM((LAYERS, *one.shape[1:]), jnp.bfloat16) for one in m]
        pairs = [pltpu.VMEM((2, LAYERS, *one.shape[1:]), jnp.bfloat16) for one in m]
        dma = lambda n: pltpu.SemaphoreType.DMA((n,))
        in_hbm, in_vmem = pl.BlockSpec(memory_space=pltpu.HBM), pl.BlockSpec(memory_space=pltpu.VMEM)
        grant = 31 << 20

        def put(marked, *results):
            shapes = [jax.ShapeDtypeStruct(x.shape, x.dtype) for x in results]
            shapes += [jax.ShapeDtypeStruct((16, 128), jnp.bfloat16)] * marked
            return pl.pallas_call(
                functools.partial(put_out, marked),
                out_shape=shapes,
                in_specs=[in_vmem] * len(results),
                out_specs=[in_hbm] * len(shapes),
                scratch_shapes=[dma(len(shapes))],
                compiler_params=pltpu.CompilerParams(vmem_limit_bytes=grant),
                name="put_out",
            )(*results)

        pieces = cut([one.shape[1] for one in m], [one.shape[2] for one in m])
        units, hops = 4 * LAYERS * len(pieces), 6 * len(pieces)
        soon = sum(a == 1 for a, _, _ in pieces)
        early = [pltpu.VMEM((LAYERS, size // 2, *one.shape[1:]), jnp.bfloat16) for one in m]
        *done, kept_up, kept_down, early_up = pl.pallas_call(
            functools.partial(kernel, size, count, pieces),
            out_shape=[*vmem(weights[:1]), *vmem(m), *vmem(v), *blocks[1:], early[1]],
            in_specs=[in_hbm] * 12,
            out_specs=[in_vmem] * 10,
            scratch_shapes=[
                *vmem(weights[1:]),
                *blocks,
                *blocks,
                *pairs,
                pltpu.VMEM((size, 8, 128), jnp.float32),
                dma(units),
                dma(3 * LAYERS * KINDS),
                dma(units),
                dma(units),
                dma(hops),
                dma(hops),
                dma(6 * soon),
                dma(6 * soon),
                dma(size - 1),
                dma(size - 1),
                pltpu.SemaphoreType.REGULAR,
            ],
            compiler_params=pltpu.CompilerParams(collective_id=0, has_side_effects=True, vmem_limit_bytes=grant),
            name="step",
        )(*(pltpu.with_memory_space_constraint(x, pltpu.HBM) for x in arrays))
        gate, *moments, after = put(1, *done)
        ends = [[(first, high) for kind, first, high in pieces if kind == a] for a in range(KINDS)]

        def finish(a, done, ahead_of, *held):
            more = ends[a + 1] if ahead_of else []
            units, hops = 4 * LAYERS * len(ends[a]), 6 * len(ends[a])
            return pl.pallas_call(
                functools.partial(gather, size, ends[a], done, more, ahead_of),
                out_shape=[*vmem(weights[a : a + 1]), *(early[a + 1 : a + 2] if more else [])],
                in_specs=[in_hbm] + [in_vmem] * (len(held) - 1),
                out_specs=[in_vmem] * (2 if more else 1),
                scratch_shapes=[
                    pltpu.SemaphoreType.REGULAR,
                    dma(units),
                    dma(units),
                    dma(hops),
                    dma(hops),
                    *([dma(6 * len(more))] * 2 if more else []),
                ],
                compiler_params=pltpu.CompilerParams(collective_id=a, has_side_effects=True, vmem_limit_bytes=grant),
                name=f"gather_{a}",
            )(*held)

        up, early_down = finish(1, 3, STAGES, after, kept_up, early_up, kept_down)
        up, after = put(1, up)
        (down,) = finish(2, STAGES, 0, after, kept_down, early_down)
        (down,) = put(0, down)
        return (gate, up, down, *moments)

    whole, cut_rows = P(None, None, None), P(None, "dp", None)
    return jax.shard_map(
        step,
        mesh=mesh,
        in_specs=(P(("rep", "dp"), None, None, None),) * 3 + (whole,) * 3 + (cut_rows,) * 6,
        out_specs=(P("rep", None, None),) * 3 + (P("rep", "dp", None),) * 6,
        check_vma=False,
    )
```
